32 devices in a mesh: lat: 4 (over z), lon: 8 (over y, x, core).
Axes of the slice: x: 2, y: 2, z: 4, core: 2. Of those that a mesh axis runs over, the one named last changes fastest.
Arguments:
- surface_forcing: float32 [4320, 1024], P('lon', 'lat'), may hold values from -40 to 40
- ocean_mask: int32 [4320, 1024], P('lon', 'lat'), may hold values 0 or 1
- self_coupling: float32 [4320, 1024], P('lon', 'lat'), may hold values from 0.2 to 2
- east_coupling: float32 [4320, 1024], P('lon', 'lat'), may hold values from 0.3 to 3
- north_coupling: float32 [4320, 1024], P('lon', 'lat'), may hold values from 0.3 to 3
- zonal_weight: float32 [1024], P('lat'), may hold values from 0.5 to 50
- aligned_inverse: float32 [8, 128, 128], P('lat'), may hold values from -1 to 4, as said below
- staggered_inverse: float32 [8, 128, 128], P('lat'), may hold values from -1 to 4, as said below
Outputs:
- solution: float32 [4320, 1024], P('lon', 'lat')
- residual: float32 [4320, 1024], P('lon', 'lat')
- direction: float32 [4320, 1024], P('lon', 'lat')
The draws below stay inside these ranges and needn't reach their ends.
Inputs may be any that keep to these rules, and one draw needn't show every extreme that they name: `aligned_inverse`: each block is symmetric and positive definite. `staggered_inverse`: each block is symmetric and positive definite.
All inputs are finite; a program needn't handle non-finite values. No bound on the sum of `ocean_mask` on one device may be relied on, other than what follows from the above.
Results may differ from the reference program's by a relative error of at most 0.00023.
Values sent between devices are 32-bit elements; how exact they have to be, the bound alone decides.
A program may use at most 64 MiB of HBM per device.

```python
import math
import jax
import jax.numpy as jnp
from jax import lax

NLON = 4320
BL = 128
NLAT = 1024
NBLK = 8


def draw_surface_forcing(key, part):
    first = jax.random.fold_in(jax.random.fold_in(key, 7), 0)
    lon_pos = jnp.arange(NLON).astype(jnp.float32) / NLON
    lat_pos = jnp.arange(NLAT).astype(jnp.float32) / NLAT
    ramp = (1.0 + 2.0 * lon_pos)[:, None] * (1.0 + 2.0 * lat_pos)[None, :]
    values = ramp * jnp.clip(jax.random.normal(first, (NLON, NLAT), jnp.float32), -4.4, 4.4)
    return values


def inverse_blocks(key, ratio, lowest, highest):
    first, second = jax.random.split(key, 2)
    index = jnp.arange(BL)
    distance = jnp.abs(index[:, None] - index[None, :]).astype(jnp.float32)
    decaying = jnp.power(jnp.float32(ratio), distance)
    mixing = jax.random.uniform(first, (NBLK, BL, BL), jnp.float32, -1.0, 1.0)
    gram = jnp.einsum('bij,bkj->bik', mixing, mixing) / (2.0 * BL)
    core = 0.5 * jnp.eye(BL, dtype=jnp.float32)[None] + decaying[None] + gram
    scales = jnp.exp(jax.random.uniform(second, (NBLK, BL), jnp.float32, jnp.log(lowest), jnp.log(highest)))
    return 0.3 * scales[:, :, None] * core * scales[:, None, :]


def draw_aligned_inverse(key, part):
    return inverse_blocks(jax.random.fold_in(key, 11), 0.6, 0.5, 2.0)


def draw_staggered_inverse(key, part):
    return inverse_blocks(jax.random.fold_in(key, 23), 0.6, 0.5, 2.0)


def place_ends(array, stream_key, smallest, high):
    extent = array.shape
    spot = [jax.random.randint(jax.random.fold_in(stream_key, axis), (), 0, extent[axis]) for axis in range(len(extent))]
    array = array.at[tuple(spot)].set(smallest)
    longest = extent.index(max(extent))
    spot[longest] = (spot[longest] + 1) % extent[longest]
    return array.at[tuple(spot)].set(high)


def shard_levels(key, extent, cuts, smallest, top_value):
    factor_of = 1.0
    for dim, shards_of in cuts:
        steps = jax.random.uniform(jax.random.fold_in(jax.random.fold_in(key, 6), dim), (shards_of,), jnp.float32, smallest / len(cuts), top_value / len(cuts))
        factor_of = factor_of * jnp.repeat(jnp.exp(steps), extent[dim] // shards_of).reshape((-1,) + (1,) * (len(extent) - 1 - dim))
    return factor_of


def setup_inputs(seed: int = 0) -> dict:
    keys = jax.random.split(jax.random.key(seed), 9)
    return {
        "surface_forcing": draw_surface_forcing(jax.random.fold_in(keys[8], 71), 0),
        "ocean_mask": place_ends((jax.random.randint(keys[1], (NLON, NLAT), 0, 5) < 4).astype(jnp.int32), jax.random.fold_in(keys[1], 1), 0, 1),
        "self_coupling": jnp.clip(jnp.exp(math.log(2.0) - 2.3025851 * jax.random.uniform(keys[2], (NLON, NLAT), jnp.float32) ** shard_levels(keys[2], (NLON, NLAT), ((0, 8), (1, 4)), -0.2, 0.2)), 0.2, 2.0),
        "east_coupling": jnp.clip(jnp.exp(math.log(3.0) - 2.3025851 * jax.random.uniform(keys[3], (NLON, NLAT), jnp.float32) ** shard_levels(keys[3], (NLON, NLAT), ((0, 8), (1, 4)), -0.2, 0.2)), 0.3, 3.0),
        "north_coupling": jnp.clip(jnp.exp(math.log(3.0) - 2.3025851 * jax.random.uniform(keys[4], (NLON, NLAT), jnp.float32) ** shard_levels(keys[4], (NLON, NLAT), ((0, 8), (1, 4)), -0.2, 0.2)), 0.3, 3.0),
        "zonal_weight": jnp.clip(jnp.exp(math.log(50.0) - 4.6051702 * jax.random.uniform(keys[5], (NLAT,), jnp.float32) ** shard_levels(keys[5], (NLAT,), ((0, 4),), -0.2, 0.2)), 0.5, 50.0),
        "aligned_inverse": draw_aligned_inverse(jax.random.fold_in(keys[8], 71), 0),
        "staggered_inverse": draw_staggered_inverse(jax.random.fold_in(keys[8], 71), 0),
    }


FULL_TURN = 6.283185307179586

def blockwise(parts, inverse):
    shaped = parts.reshape(2, NLON, NBLK, BL)
    result = jnp.einsum('bij,smbj->smbi', inverse, shaped, precision=lax.Precision.HIGHEST)
    return result.reshape(2, NLON, NLAT)

def staggered(parts, inverse):
    half = BL // 2
    zeros = jnp.zeros((2, NLON, half), parts.dtype)
    moved = jnp.concatenate([parts[:, :, half:], zeros], axis=2)
    result = blockwise(moved, inverse)
    return jnp.concatenate([zeros, result[:, :, :NLAT - half]], axis=2)

def precondition(field, wet, zonal_weight, aligned_inverse, staggered_inverse):
    spectrum = jnp.fft.fft(field, axis=0)
    modes = jnp.arange(NLON).astype(jnp.float32)
    wave = 2.0 - 2.0 * jnp.cos(FULL_TURN * modes / NLON)
    scale = lax.rsqrt(1.0 + zonal_weight[None, :] * wave[:, None])
    parts = jnp.stack([spectrum.real, spectrum.imag]) * scale
    combined = (blockwise(parts, aligned_inverse) + staggered(parts, staggered_inverse)) * scale
    back = jnp.fft.ifft(combined[0] + 1j * combined[1], axis=0).real
    return wet * back

def reference(surface_forcing, ocean_mask, self_coupling, east_coupling, north_coupling, zonal_weight, aligned_inverse, staggered_inverse):
    wet = ocean_mask.astype(jnp.float32)
    row_index = jnp.arange(NLAT)
    top_flag = jnp.where(row_index < NLAT - 1, 1.0, 0.0).astype(jnp.float32)
    east = east_coupling * wet * jnp.roll(wet, -1, axis=0)
    north = north_coupling * wet * jnp.roll(wet, -1, axis=1) * top_flag[None, :]
    west = jnp.roll(east, 1, axis=0)
    south = jnp.roll(north, 1, axis=1)

    def operate(field):
        result = (1.0 - wet) * field + wet * self_coupling * field
        result = result + east * (field - jnp.roll(field, -1, axis=0))
        result = result + west * (field - jnp.roll(field, 1, axis=0))
        result = result + north * (field - jnp.roll(field, -1, axis=1))
        result = result + south * (field - jnp.roll(field, 1, axis=1))
        return result
    rhs_wet = wet * surface_forcing
    first = precondition(rhs_wet, wet, zonal_weight, aligned_inverse, staggered_inverse)
    rz_now = jnp.sum(rhs_wet * first)
    image = operate(first)
    curvature = jnp.sum(first * image)
    alpha = rz_now / curvature
    solution = alpha * first
    residual = rhs_wet - alpha * image
    second = precondition(residual, wet, zonal_weight, aligned_inverse, staggered_inverse)
    rz_next = jnp.sum(residual * second)
    direction = second + rz_next / rz_now * first
    return (solution, residual, direction)
```

```python
import functools

import jax
import jax.numpy as jnp
import numpy as np
from jax import lax
from jax.experimental import pallas as pl
from jax.experimental.pallas import tpu as pltpu
from jax.sharding import PartitionSpec as P

MESH = pl.DeviceIdType.MESH


def outer_table(groups):
    table = np.zeros((groups, groups))
    place = np.arange(groups)
    table[0] = 1.0
    table[1] = np.where(place % 2 == 0, 1.0, -1.0)
    for mode in range(1, groups // 2):
        turn = 2.0 * np.pi * (mode * place % groups) / groups
        table[2 * mode] = np.cos(turn)
        table[2 * mode + 1] = -np.sin(turn)
    table[np.abs(table) < 1e-12] = 0.0
    return table


def inner_tables(groups, length, padded):
    total = groups * length
    pairs = groups // 2
    matrix = np.zeros((pairs, 2 * padded, 2 * padded))
    waves = np.zeros((pairs, 2 * padded))
    cell = np.arange(length)

    def turns(modes):
        return 2.0 * np.pi * (modes[:, None] * cell[None, :] % total) / total

    def note(pair, start, modes):
        stop = start + len(modes)
        waves[pair, start:stop] = 2.0 - 2.0 * np.cos(2.0 * np.pi * modes / total)

    for part, (first, real_count) in enumerate(((0, length // 2 + 1), (groups // 2, (length + 1) // 2))):
        skipped = 1 if part == 0 else 0
        real = first + groups * np.arange(real_count)
        imag = first + groups * (skipped + np.arange(length - real_count))
        row = part * padded
        columns = slice(part * padded, part * padded + length)
        matrix[0, row : row + real_count, columns] = np.cos(turns(real))
        matrix[0, row + real_count : row + length, columns] = -np.sin(turns(imag))
        note(0, row, real)
        note(0, row + real_count, imag)
    for pair in range(1, pairs):
        modes = pair + groups * np.arange(length)
        angle = turns(modes)
        low, high = slice(0, length), slice(padded, padded + length)
        matrix[pair, low, low] = np.cos(angle)
        matrix[pair, low, high] = np.sin(angle)
        matrix[pair, high, low] = -np.sin(angle)
        matrix[pair, high, high] = np.cos(angle)
        note(pair, 0, modes)
        note(pair, padded, modes)
    single = matrix.astype(np.float32)
    leading = single.astype(jnp.bfloat16)
    rest = (matrix - leading.astype(np.float64)).astype(jnp.bfloat16)
    return np.stack([leading, rest], axis=1), waves.astype(np.float32)


def parted(value):
    leading = value.astype(jnp.bfloat16)
    return leading, (value - leading.astype(jnp.float32)).astype(jnp.bfloat16)


def dot(left, right):
    return jnp.dot(left, right, preferred_element_type=jnp.float32)


def weighted(values, factors):
    total = None
    for value, factor in zip(values, factors):
        if factor == 0.0:
            continue
        term = value if factor == 1.0 else value * np.float32(factor)
        total = term if total is None else total + term
    return total


class Plan:
    def __init__(self, groups, bands, length, columns, block, width_of):
        self.groups, self.bands, self.length = groups, bands, length
        self.pairs = groups // 2
        self.columns, self.block = columns, block
        self.chunk, self.padded = width_of
        self.width = 2 * self.padded
        self.rows = max(-(-length // 128) * 128, -(-self.padded // 128) * 128)
        self.tile = next(t for t in (384, 256, 128) if self.width % t == 0)
        self.table = outer_table(groups)

    def scratch(self):
        f32, bf16 = jnp.float32, jnp.bfloat16
        G, NP, C, PD, W, R, L = (
            self.groups, self.pairs, self.chunk, self.padded, self.width, self.rows, self.block
        )
        vmem, dma = pltpu.VMEM, pltpu.SemaphoreType.DMA
        return {
            "forcing": vmem((self.length, 2 * L), f32),
            "mask": vmem((self.length, 2 * L), jnp.int32),
            "selfc": vmem((self.length, 2 * L), f32),
            "eastc": vmem((self.length, 2 * L), f32),
            "northc": vmem((self.length, 2 * L), f32),
            "zonal": vmem((1, 2 * L), f32),
            "zonal_in": vmem((2, 1, 2 * L), f32),
            "aligned": vmem((2, L, L), f32),
            "staggered": vmem((2, L, L), f32),
            "carried": vmem((L, L), f32),
            "matrix": vmem((2, W, W), bf16),
            "turned": vmem((2, W, W), bf16),
            "wave": vmem((W, L), f32),
            "wet": vmem((2, R + 16, L), f32),
            "east_wet": vmem((2, R, L), f32),
            "east": vmem((2, R + 16, L), f32),
            "north": vmem((2, R, L), f32),
            "south": vmem((2, R, L), f32),
            "diag": vmem((2, R, L), f32),
            "field": vmem((2, R + 16, L), f32),
            "row_in": vmem((3, 2, 8, L), f32),
            "row_out": vmem((3, 2, 8, L), f32),
            "edge_out": vmem((2, 2, 8, L), f32),
            "edge_in": vmem((2, 2, 8, L), f32),
            "scale": vmem((3, W, L), f32),
            "scale_out": vmem((W, L), f32),
            "gain": vmem((2, 2 * L, L), bf16),
            "gain_z": vmem((2, L, L), bf16),
            "xs": vmem((2, 2, R, L), f32),
            "got1": vmem((2, 2, G, C, L), f32),
            "send2": vmem((2, NP, 2, 2, C, L), f32),
            "got2": vmem((2, 2, PD, L), f32),
            "mate2": vmem((2, 2, PD, L), f32),
            "zs": vmem((2, 2, PD, L), f32),
            "zgot": vmem((2, 2, PD, L), f32),
            "spec": vmem((2, W, L), f32),
            "spec_mate": vmem((W, L), f32),
            "spec_z": vmem((W, L), f32),
            "mixed": vmem((2, W, L), f32),
            "send3": vmem((2, 2, PD, L), f32),
            "got3": vmem((2, G, 2, C, L), f32),
            "send4": vmem((2, G, 2, C, L), f32),
            "got4": vmem((2, 2, R, L), f32),
            "ew": vmem((2, 2, 8, L), f32),
            "part": vmem((2, 2, 8, L), f32),
            "red1": vmem((2, G, 2, 8, L), f32),
            "middle": vmem((2, 2, 8, L), f32),
            "red2": vmem((2, self.bands, 2, 8, L), f32),
            "out": vmem((3, self.length, 2 * L), f32),
            "load": dma((16,)),
            "s1": dma((2, 2, NP, 2)),
            "r1": dma((2, 2, NP, 2)),
            "s2": dma((2, 2, NP, 2)),
            "r2": dma((2, NP, 2)),
            "sm": dma((2, NP, 2)),
            "rm": dma((2, NP, 2)),
            "sz": dma((2, 2, NP, 2)),
            "rz": dma((2, 2, NP, 2)),
            "s3": dma((2, NP, 2)),
            "r3": dma((2, NP, 2)),
            "s4": dma((2, 2, NP, 2)),
            "r4": dma((2, 2, NP, 2)),
            "sw": dma((2, 2, NP, 2)),
            "rw": dma((2, 2)),
            "srow": dma((3, 2)),
            "rrow": dma((3, 2)),
            "sedge": dma((2, 2)),
            "redge": dma((2, 2)),
            "szon": dma((2,)),
            "rzon": dma((2,)),
            "sstag": dma,
            "rstag": dma,
            "sa": dma((2, NP, 2)),
            "ra": dma((2, NP, 2)),
            "sb": dma((2, self.bands)),
            "rb": dma((2, self.bands)),
            "store": dma((3,)),
        }


class Refs:
    pass


def kernel(plan, names, *refs):
    (forcing_ref, mask_ref, self_ref, east_ref, north_ref, zonal_ref, aligned_ref, staggered_ref,
     matrix_ref, wave_ref, solution_ref, residual_ref, direction_ref) = refs[:13]
    s = Refs()
    for name, ref in zip(names, refs[13:]):
        setattr(s, name, ref)
    G, NP, C, PD, W, R, L = (
        plan.groups, plan.pairs, plan.chunk, plan.padded, plan.width, plan.rows, plan.block
    )
    bands, length, tile, table = plan.bands, plan.length, plan.tile, plan.table
    half = L // 2
    total = G * length
    f32 = jnp.float32
    band = lax.axis_index("lat")
    me = lax.axis_index("lon")
    pair, core = me // 2, me % 2
    mate = me + 1 - 2 * core
    has_up, has_down = band < bands - 1, band > 0
    STEPS = [(d, e) for d in range(1, NP) for e in (0, 1)] + [(0, 1)]
    last_chunk = (length - 1) // C
    last_tile = (length - 1) // 8 * 8
    last_row = (length - 1) % 8

    def to_dev(d, e):
        return 2 * ((pair + d) % NP) + (core + e) % 2

    def from_dev(d, e):
        return 2 * ((pair - d + NP) % NP) + (core + e) % 2

    def remote(src, dst, send, recv, device):
        return pltpu.make_async_remote_copy(
            src_ref=src, dst_ref=dst, send_sem=send, recv_sem=recv,
            device_id=device, device_id_type=MESH,
        )

    pending = []

    def launch(make, when=None):
        if when is None:
            make().start()
        else:
            pl.when(when)(lambda: make().start())
        pending.append((make, when))

    def await_recv(make, when=None):
        if when is None:
            make().wait_recv()
        else:
            pl.when(when)(lambda: make().wait_recv())

    def rows(index):
        return pl.ds(pl.multiple_of(index * C, 8), C)

    def span(index, size=128):
        return pl.ds(pl.multiple_of(index * size, size), size)

    def loop(count, body):
        def step(index, carry):
            body(index)
            return carry
        lax.fori_loop(0, count, step, 0)

    def eight_on(start, count):
        return pl.ds(start + 8 if isinstance(start, int) else pl.multiple_of(start + 8, 8), count)

    def loop_rows(body):
        full = length // 128
        loop(full, lambda index: body(pl.multiple_of(index * 128, 128), 128))
        if length % 128:
            body(full * 128, length % 128)

    def lanes_left(count):
        return lax.broadcasted_iota(jnp.int32, (count, L), 1) < half

    def groups_of(t0, t1):
        mask = lanes_left(t0.shape[0])
        return jnp.where(mask, t1, t0), jnp.where(mask, t0, t1)

    loads = []
    for index, (src, dst) in enumerate((
        (forcing_ref, s.forcing),
        (mask_ref, s.mask),
        (matrix_ref.at[pair], s.matrix),
        (wave_ref.at[pair], s.wave),
        (self_ref, s.selfc),
        (east_ref, s.eastc),
        (north_ref, s.northc),
        (zonal_ref, s.zonal),
        (aligned_ref, s.aligned),
        (staggered_ref, s.staggered),
    )):
        loads.append(pltpu.make_async_copy(src, dst, s.load.at[index]))
        loads[-1].start()

    barrier = pltpu.get_barrier_semaphore()
    for d, e in STEPS:
        pl.semaphore_signal(barrier, inc=1, device_id=(band, to_dev(d, e)), device_id_type=MESH)
    for step in range(1, bands):
        pl.semaphore_signal(
            barrier, inc=1, device_id=((band + step) % bands, me), device_id_type=MESH
        )

    loads[0].wait()
    loads[1].wait()
    s.xs[0, :, length:R, :] = jnp.zeros((2, R - length, L), f32)
    s.wet[:, 8 + length : 16 + R, :] = jnp.zeros((2, R + 8 - length, L), f32)
    s.field[:, 8 + R : 16 + R, :] = jnp.zeros((2, 8, L), f32)

    def make_rhs(start, count):
        at = pl.ds(start, count)
        wet = s.mask[at, :].astype(f32)
        rhs = wet * s.forcing[at, :]
        a, b = groups_of(rhs[:, :L], rhs[:, L:])
        s.xs[0, 0, at, :] = a
        s.xs[0, 1, at, :] = b
        at8 = eight_on(start, count)
        s.wet[0, at8, :] = wet[:, :L]
        s.wet[1, at8, :] = wet[:, L:]

    loop_rows(make_rhs)
    pl.semaphore_wait(barrier, G + bands - 2)

    def send_phase1(t, g):
        for d, e in STEPS:
            launch(functools.partial(
                lambda d, e: remote(
                    s.xs.at[t, g, rows(to_dev(d, e))], s.got1.at[t, g, me],
                    s.s1.at[t, g, d, e], s.r1.at[t, g, d, e], (band, to_dev(d, e))), d, e))
        s.got1[t, g, me] = s.xs[t, g, rows(me), :]

    def outer_forward(t, g):
        for d, e in STEPS:
            origin = from_dev(d, e)
            remote(s.xs.at[t, g, rows(origin)], s.got1.at[t, g, origin],
                   s.s1.at[t, g, d, e], s.r1.at[t, g, d, e], (band, origin)).wait_recv()

        def step(index):
            at = span(index, 8)
            values = [s.got1[t, g, place, at, :] for place in range(G)]
            for row in range(G):
                s.send2[t, row // 2, g, row % 2, at, :] = weighted(values, table[row])

        loop(C // 8, step)
        e = (g + core) % 2
        for d in list(range(1, NP)) + [0]:
            target = 2 * ((pair + d) % NP) + g
            launch(functools.partial(
                lambda d, target: remote(
                    s.send2.at[t, (pair + d) % NP, g], s.got2.at[t, :, rows(me), :],
                    s.s2.at[t, g, d, e], s.r2.at[t, d, e], (band, target)), d, target),
                None if d else core != g)

        @pl.when(core == g)
        def _():
            s.got2[t, :, rows(me), :] = s.send2[t, pair, g]

    def forward_on(t, d, e):
        origin = from_dev(d, e)
        at = rows(origin)
        launch(functools.partial(
            lambda at, d, e: remote(
                s.got2.at[t, :, at, :], s.mate2.at[t, :, at, :],
                s.sm.at[t, d, e], s.rm.at[t, d, e], (band, mate)), at, d, e))

        @pl.when(core == 1)
        def _():
            low, high = s.got2[t, 0, at, :], s.got2[t, 1, at, :]
            mask = lanes_left(C)
            s.zs[t, 0, at, :] = jnp.where(mask, low, pltpu.roll(high, half, 1))
            s.zs[t, 1, at, :] = jnp.where(mask, pltpu.roll(low, half, 1), high)

        launch(functools.partial(
            lambda at, d, e: remote(
                s.zs.at[t, 0, at, :], s.zgot.at[t, 0, at, :],
                s.sz.at[t, 0, d, e], s.rz.at[t, 0, d, e], (band - 1, me)), at, d, e),
            (core == 1) & has_down)
        launch(functools.partial(
            lambda at, d, e: remote(
                s.zs.at[t, 1, at, :], s.zgot.at[t, 1, at, :],
                s.sz.at[t, 1, d, e], s.rz.at[t, 1, d, e], (band + 1, me)), at, d, e),
            (core == 1) & has_up)

    def relay(t):
        forward_on(t, 0, 0)
        for d, e in [(0, 1)] + [step for step in STEPS if step[0]]:
            origin = from_dev(d, e)
            remote(s.send2.at[t, 0, 0], s.got2.at[t, :, rows(origin), :],
                   s.s2.at[t, 0, d, e], s.r2.at[t, d, e], (band, origin)).wait_recv()
            forward_on(t, d, e)

    def wait_mate(t):
        for d, e in [(0, 0)] + STEPS:
            at = rows(2 * ((pair - d + NP) % NP) + (1 - core + e) % 2)
            remote(s.got2.at[t, :, at, :], s.mate2.at[t, :, at, :],
                   s.sm.at[t, d, e], s.rm.at[t, d, e], (band, mate)).wait_recv()

    def transform(source, scale, put):
        hi, lo = parted(source)
        both = jnp.concatenate([hi, lo], axis=1)

        def step(index):
            at = span(index, tile)
            wide = dot(s.matrix[0, at, :], both)
            value = wide[:, :L] + (wide[:, L:] + dot(s.matrix[1, at, :], hi))
            put(at, value * scale[at, :])

        loop(W // tile, step)

    def put_in(ref):
        def put(at, value):
            ref[at, :] = value
        return put

    def own_spectrum(t):
        transform(s.got2[t].reshape(W, L), s.scale.at[0], put_in(s.spec.at[t]))

    def mate_spectrum(t):
        transform(s.mate2[t].reshape(W, L), s.scale.at[1], put_in(s.spec_mate))

    def mix(t):
        def step(index):
            at = span(index, tile)
            hi, lo = parted(jnp.concatenate([s.spec[t, at, :], s.spec_mate[at, :]], axis=1))
            s.mixed[t, at, :] = dot(hi, s.gain[0]) + (dot(lo, s.gain[0]) + dot(hi, s.gain[1]))

        loop(W // tile, step)

        @pl.when(core == 1)
        def _():
            for d, e in [(0, 0)] + STEPS:
                for way, has in ((0, has_up), (1, has_down)):
                    def wait(way=way, d=d, e=e):
                        at = rows(from_dev(d, e))
                        remote(s.zs.at[t, way, at, :], s.zgot.at[t, way, at, :],
                               s.sz.at[t, way, d, e], s.rz.at[t, way, d, e],
                               (band + 1 - 2 * way, me)).wait_recv()
                    pl.when(has)(wait)
            above, below = s.zgot[t, 0], s.zgot[t, 1]
            mask = lanes_left(PD)
            cells = jnp.concatenate([
                jnp.where(mask, above, pltpu.roll(below, half, 1)),
                jnp.where(mask, pltpu.roll(above, half, 1), below)], axis=0)

            def put(at, value):
                hi, lo = parted(value)
                s.mixed[t, at, :] = s.mixed[t, at, :] + (
                    dot(hi, s.gain_z[0]) + (dot(lo, s.gain_z[0]) + dot(hi, s.gain_z[1])))

            transform(cells, s.scale.at[2], put)

    def inner_back(t):
        hi, lo = parted(s.mixed[t] * s.scale_out[...])
        both = jnp.concatenate([hi, lo], axis=1)
        size = G // 2 * C
        first = 1 - me // (G // 2)
        for turn in range(2):
            side = first if turn == 0 else 1 - first
            for part in range(2):
                at = pl.ds(pl.multiple_of(part * PD + side * size, 16), size)
                wide = dot(s.turned[0, at, :], both)
                s.send3[t, part, pl.ds(pl.multiple_of(side * size, 8), size), :] = (
                    wide[:, :L] + (wide[:, L:] + dot(s.turned[1, at, :], hi)))
            for d, e in STEPS:
                to = to_dev(d, e)
                launch(functools.partial(
                    lambda d, e, to: remote(
                        s.send3.at[t, :, rows(to), :], s.got3.at[t, me],
                        s.s3.at[t, d, e], s.r3.at[t, d, e], (band, to)), d, e, to),
                    to // (G // 2) == side)
        s.got3[t, me] = s.send3[t, :, rows(me), :]

    def outer_back(t, g, edges):
        e = (g + core) % 2
        for d in range(NP):
            origin = 2 * ((pair - d + NP) % NP) + g
            await_recv(functools.partial(
                lambda d, origin: remote(
                    s.send3.at[t, :, rows(0), :], s.got3.at[t, origin],
                    s.s3.at[t, d, e], s.r3.at[t, d, e], (band, origin)), d, origin),
                None if d else core != g)

        def step(index):
            at = span(index, 8)
            values = [s.got3[t, 2 * (row // 2) + g, row % 2, at, :] for row in range(G)]
            for place in range(G):
                s.send4[t, place, g, at, :] = weighted(values, table[:, place])

        loop(C // 8, step)
        for d, e in STEPS:
            launch(functools.partial(
                lambda d, e: remote(
                    s.send4.at[t, to_dev(d, e), g], s.got4.at[t, g, rows(me), :],
                    s.s4.at[t, g, d, e], s.r4.at[t, g, d, e], (band, to_dev(d, e))), d, e))
        s.got4[t, g, rows(me), :] = s.send4[t, me, g]
        if not edges:
            return
        for way, (owner, shift, at) in enumerate((
            (0, 1, 0), (last_chunk, G - 1, (length - 1) % C // 8 * 8))):
            for d, e in STEPS:
                launch(functools.partial(
                    lambda way, shift, at, d, e: remote(
                        s.send4.at[t, (to_dev(d, e) + shift) % G, g, pl.ds(at, 8), :], s.ew.at[way, g],
                        s.sw.at[way, g, d, e], s.rw.at[way, g], (band, to_dev(d, e))),
                    way, shift, at, d, e), me == owner)

            @pl.when(me == owner)
            def _(way=way, shift=shift, at=at):
                s.ew[way, g] = s.send4[t, (me + shift) % G, g, pl.ds(at, 8), :]

    def wait_back(t, g, edges):
        for d, e in STEPS:
            origin = from_dev(d, e)
            remote(s.send4.at[t, 0, g], s.got4.at[t, g, rows(origin), :],
                   s.s4.at[t, g, d, e], s.r4.at[t, g, d, e], (band, origin)).wait_recv()
        if edges:
            for way, owner in enumerate((0, last_chunk)):
                await_recv(functools.partial(
                    lambda way: remote(
                        s.send4.at[t, 0, g, pl.ds(0, 8), :], s.ew.at[way, g],
                        s.sw.at[way, g, 0, 1], s.rw.at[way, g], (band, mate)), way), me != owner)

    def send_edges(i):
        for way, (device, has) in enumerate((((band - 1, me), has_down), ((band + 1, me), has_up))):
            launch(functools.partial(
                lambda way, device: remote(
                    s.edge_out.at[i, way], s.edge_in.at[i, way],
                    s.sedge.at[i, way], s.redge.at[i, way], device), way, device), has)

    def wait_edges(i):
        for way, has in enumerate((has_up, has_down)):
            await_recv(functools.partial(
                lambda way: remote(
                    s.edge_out.at[i, way], s.edge_in.at[i, way],
                    s.sedge.at[i, way], s.redge.at[i, way], (band + 1 - 2 * way, me)), way), has)

    def column_of(i, way):
        tile8 = s.edge_in[i, way]
        return jnp.concatenate([tile8, jnp.zeros((L - 8, L), f32)], axis=0).T

    def reduce_send(i):
        for d, e in STEPS:
            launch(functools.partial(
                lambda d, e: remote(
                    s.part.at[i], s.red1.at[i, me], s.sa.at[i, d, e], s.ra.at[i, d, e],
                    (band, to_dev(d, e))), d, e))
        s.red1[i, me] = s.part[i]

    def reduce_middle(i):
        for d, e in STEPS:
            origin = from_dev(d, e)
            remote(s.part.at[i], s.red1.at[i, origin], s.sa.at[i, d, e], s.ra.at[i, d, e],
                   (band, origin)).wait_recv()
        value = s.red1[i, 0]
        for place in range(1, G):
            value = value + s.red1[i, place]
        s.middle[i] = value
        s.red2[i, band] = value
        for step in range(1, bands):
            launch(functools.partial(
                lambda step: remote(
                    s.middle.at[i], s.red2.at[i, band], s.sb.at[i, step], s.rb.at[i, step],
                    ((band + step) % bands, me)), step))

    def reduce_end(i):
        for step in range(1, bands):
            origin = (band - step + bands) % bands
            remote(s.middle.at[i], s.red2.at[i, origin], s.sb.at[i, step], s.rb.at[i, step],
                   (origin, me)).wait_recv()
        value = s.red2[i, 0]
        for place in range(1, bands):
            value = value + s.red2[i, place]
        return [jnp.sum(value[k], keepdims=True) for k in range(2)]

    def eights(value):
        return value.reshape(value.shape[0] // 8, 8, L).sum(axis=0)

    def weight_of(at):
        wave = s.wave[at, :]
        edge = (wave == 0.0) | (wave == 4.0)
        return jnp.where(edge, np.float32(1.0 / total), np.float32(2.0 / total))

    send_phase1(0, 1)
    send_phase1(0, 0)

    blocks = R // 128

    def shifted(index, by=8):
        return pl.ds(pl.multiple_of(index * 128 + by, 8), 128)

    for load in loads[4:]:
        load.wait()
    for ref in (s.east_wet, s.north):
        ref[:, length:R, :] = jnp.zeros((2, R - length, L), f32)

    def make_faces(start, count):
        at, at8 = pl.ds(start, count), eight_on(start, count)
        for k in range(2):
            lanes = slice(k * L, (k + 1) * L)
            wet = s.wet[k, at8, :]
            s.east_wet[k, at, :] = s.eastc[at, lanes] * wet
            s.north[k, at, :] = s.northc[at, lanes] * wet

    loop_rows(make_faces)
    west_dev, east_dev = (me + G - 1) % G, (me + 1) % G
    s.row_out[0] = s.wet[:, 8:16, :]
    s.row_out[1] = s.wet[:, 8 + last_tile : 16 + last_tile, :]
    s.row_out[2] = s.east_wet[:, last_tile : last_tile + 8, :]
    for k, device in enumerate((west_dev, east_dev, east_dev)):
        src = s.row_out.at[k]
        launch(functools.partial(
            lambda k, src, device: remote(
                src, s.row_in.at[k], s.srow.at[k, 0], s.rrow.at[k, 0], (band, device)), k, src, device))

    def take_edges(i, low, high, by):
        for b in range(blocks):
            s.edge_out[i, 0, b : b + 1, :] = low[pl.ds(128 * b + by[0], 128), :].T[:1, :]
            s.edge_out[i, 1, b : b + 1, :] = high[pl.ds(128 * b + by[1], 128), :].T[L - 1 :, :]
        if blocks < 8:
            s.edge_out[i, :, blocks:, :] = jnp.zeros((2, 8 - blocks, L), f32)

    take_edges(0, s.wet.at[0], s.north.at[1], (8, 0))
    send_edges(0)
    for way, (device, has) in enumerate((((band - 1, me), has_down), ((band + 1, me), has_up))):
        launch(functools.partial(
            lambda way, device: remote(
                s.zonal, s.zonal_in.at[way], s.szon.at[way], s.rzon.at[way], device), way, device), has)

    def send_stag():
        return remote(s.staggered.at[1], s.carried, s.sstag, s.rstag, (band + 1, me))

    launch(send_stag, has_up)
    for way, has in enumerate((has_up, has_down)):
        @pl.when(jnp.logical_not(has))
        def _(way=way):
            for i in range(2):
                s.edge_in[i, way] = jnp.zeros((8, L), f32)
                s.zgot[i, way] = jnp.zeros((PD, L), f32)
            s.zonal_in[way] = jnp.zeros((1, 2 * L), f32)

    @pl.when(jnp.logical_not(has_down))
    def _():
        s.carried[...] = jnp.zeros((L, L), f32)

    loads[2].wait()
    loads[3].wait()

    def turn(index):
        at = span(index)
        for k in range(2):
            s.turned[k, at, :] = s.matrix[k, :, at].T

    loop(W // 128, turn)

    outer_forward(0, 1)
    outer_forward(0, 0)

    for way, has in enumerate((has_up, has_down)):
        await_recv(functools.partial(
            lambda way: remote(
                s.zonal, s.zonal_in.at[way], s.szon.at[way], s.rzon.at[way],
                (band + 1 - 2 * way, me)), way), has)
    z0, z1 = s.zonal[:, :L], s.zonal[:, L:]
    mask1 = lanes_left(1)
    zone_a, zone_b = jnp.where(mask1, z1, z0), jnp.where(mask1, z0, z1)
    is_low = core == 0
    zones = (
        jnp.where(is_low, zone_a, zone_b),
        jnp.where(is_low, zone_b, zone_a),
        jnp.where(mask1, s.zonal_in[0, :, :L], s.zonal_in[1, :, L:]),
    )

    def make_scale(index):
        at = span(index)
        wave = s.wave[at, :]
        for k, zone in enumerate(zones):
            s.scale[k, at, :] = lax.rsqrt(1.0 + wave * zone)
        s.scale_out[at, :] = s.scale[0, at, :] * weight_of(at)

    loop(W // 128, make_scale)

    @pl.when(has_down)
    def _():
        remote(s.staggered.at[1], s.carried, s.sstag, s.rstag, (band - 1, me)).wait_recv()

    def swapped(value):
        value = jnp.concatenate([value[half:, :], value[:half, :]], axis=0)
        return pltpu.roll(value, half, 1)

    row_top = lax.broadcasted_iota(jnp.int32, (L, L), 0) < half
    col_left = lanes_left(L)
    tl, tr = row_top & col_left, row_top & jnp.logical_not(col_left)
    bl = jnp.logical_not(row_top) & col_left
    br = jnp.logical_not(row_top) & jnp.logical_not(col_left)
    al0, al1 = s.aligned[0], s.aligned[1]
    mid, top, low = swapped(s.staggered[0]), swapped(s.staggered[1]), swapped(s.carried[...])
    zero = jnp.zeros((L, L), f32)

    def pick(*items):
        value = zero
        for where, block in items:
            value = jnp.where(where, block, value)
        return value

    own = jnp.where(
        is_low, mid + pick((tl, al1), (br, al0)), pick((tl, al0 + low), (br, al1 + top)))
    beside = jnp.where(is_low, pick((tr, al0), (bl, al1)), pick((tr, al1), (bl, al0)))
    across = pick((tr, top), (bl, low))
    for k, value in enumerate((own, beside)):
        hi, lo = parted(value)
        s.gain[0, k * L : (k + 1) * L, :] = hi
        s.gain[1, k * L : (k + 1) * L, :] = lo
    hi, lo = parted(across)
    s.gain_z[0] = hi
    s.gain_z[1] = lo

    relay(0)
    own_spectrum(0)
    wait_mate(0)
    mate_spectrum(0)
    mix(0)
    inner_back(0)

    def rz_part(index, carry):
        at = span(index)
        return carry + eights(s.spec[0, at, :] * (s.mixed[0, at, :] * weight_of(at)))

    s.part[0, 0] = lax.fori_loop(0, W // 128, rz_part, jnp.zeros((8, L), f32))

    for k, device in enumerate((east_dev, west_dev, west_dev)):
        remote(s.row_out.at[k], s.row_in.at[k], s.srow.at[k, 0], s.rrow.at[k, 0], (band, device)).wait_recv()
    wait_edges(0)
    north_col, south_col = column_of(0, 0), column_of(0, 1)
    for k in range(2):
        s.wet[k, 8 + length : 9 + length, :] = s.row_in[0, k, 0:1, :]
        s.east[k, 7:8, :] = s.row_in[2, k, last_row : last_row + 1, :] * s.wet[k, 8:9, :]
    lane = lax.broadcasted_iota(jnp.int32, (128, L), 1)
    first_lane, last_lane = lane == 0, lane == L - 1
    for b in range(blocks):
        at, at8, at9 = pl.ds(128 * b, 128), pl.ds(128 * b + 8, 128), pl.ds(128 * b + 9, 128)
        wet = [s.wet[k, at8, :] for k in range(2)]
        east = [s.east_wet[k, at, :] * s.wet[k, at9, :] for k in range(2)]
        moved = [pltpu.roll(value, L - 1, 1) for value in wet]
        beyond = jnp.broadcast_to(north_col[:, b : b + 1], (128, L))
        north = [
            s.north[0, at, :] * jnp.where(last_lane, moved[1], moved[0]),
            s.north[1, at, :] * jnp.where(last_lane, beyond, moved[1]),
        ]
        moved = [pltpu.roll(value, 1, 1) for value in north]
        beyond = jnp.broadcast_to(south_col[:, b : b + 1], (128, L))
        south = [
            jnp.where(first_lane, beyond * wet[0], moved[0]),
            jnp.where(first_lane, moved[0], moved[1]),
        ]
        for k in range(2):
            s.east[k, at8, :] = east[k]
            s.north[k, at, :] = north[k]
            s.south[k, at, :] = south[k]
    def make_diag(start, count):
        at, at8 = pl.ds(start, count), eight_on(start, count)
        for k in range(2):
            wet = s.wet[k, at8, :]
            own = (1.0 - wet) + wet * s.selfc[at, k * L : (k + 1) * L]
            s.diag[k, at, :] = own + s.diag[k, at, :]

    for b in range(blocks):
        at, at8, at7 = pl.ds(128 * b, 128), pl.ds(128 * b + 8, 128), pl.ds(128 * b + 7, 128)
        for k in range(2):
            s.diag[k, at, :] = (
                (s.east[k, at8, :] + s.east[k, at7, :]) + (s.north[k, at, :] + s.south[k, at, :]))
    s.diag[:, length:R, :] = jnp.zeros((2, R - length, L), f32)
    loop_rows(make_diag)
    if R > PD:
        for t in range(2):
            for g in range(2):
                s.got4[t, g, PD:, :] = jnp.zeros((R - PD, L), f32)

    outer_back(0, 0, True)
    outer_back(0, 1, True)
    wait_back(0, 0, True)
    wait_back(0, 1, True)

    def fields_of(t, at, count):
        a, b = s.got4[t, 0, at, :], s.got4[t, 1, at, :]
        mask = lanes_left(count)
        return jnp.where(mask, b, a), jnp.where(mask, a, b)

    def make_field(index):
        at8 = shifted(index)
        for k, value in enumerate(fields_of(0, span(index), 128)):
            s.field[k, at8, :] = s.wet[k, at8, :] * value

    loop(blocks, make_field)
    take_edges(1, s.field.at[0], s.field.at[1], (8, 8))
    send_edges(1)
    mask1 = lanes_left(1)
    for way, (row, source) in enumerate(((0, 0), (last_row, 1))):
        a, b = s.ew[way, 0, row : row + 1, :], s.ew[way, 1, row : row + 1, :]
        for k, value in enumerate((jnp.where(mask1, b, a), jnp.where(mask1, a, b))):
            at = 8 + length if way == 0 else 7
            s.field[k, at : at + 1, :] = s.row_in[source, k, row : row + 1, :] * value

    curvature = jnp.zeros((8, L), f32)
    for b in range(blocks):
        at, at8 = pl.ds(128 * b, 128), pl.ds(128 * b + 8, 128)
        at7, at9 = pl.ds(128 * b + 7, 128), pl.ds(128 * b + 9, 128)
        here = [s.field[k, at8, :] for k in range(2)]
        up = [pltpu.roll(value, L - 1, 1) for value in here]
        down = [pltpu.roll(value, 1, 1) for value in here]
        up = [jnp.where(last_lane, up[1], up[0]), jnp.where(last_lane, 0.0, up[1])]
        down = [jnp.where(first_lane, 0.0, down[0]), jnp.where(first_lane, down[0], down[1])]
        image = []
        for k in range(2):
            value = s.diag[k, at, :] * here[k]
            value = value - s.east[k, at8, :] * s.field[k, at9, :]
            value = value - s.east[k, at7, :] * s.field[k, at7, :]
            value = value - s.north[k, at, :] * up[k]
            value = value - s.south[k, at, :] * down[k]
            if 128 * (b + 1) > length:
                row = lax.broadcasted_iota(jnp.int32, (128, L), 0)
                value = jnp.where(row < length - 128 * b, value, 0.0)
            image.append(value)
            curvature = curvature + eights(here[k] * image[k])
        s.xs[1, 0, at, :], s.xs[1, 1, at, :] = groups_of(*image)

    send_phase1(1, 0)
    wait_edges(1)
    north_col, south_col = column_of(1, 0), column_of(1, 1)
    for b in range(blocks):
        at, at8 = pl.ds(128 * b, 128), pl.ds(128 * b + 8, 128)
        south = s.south[0, at, :] * jnp.broadcast_to(south_col[:, b : b + 1], (128, L))
        north = s.north[1, at, :] * jnp.broadcast_to(north_col[:, b : b + 1], (128, L))
        extra = jnp.where(first_lane, south, jnp.where(last_lane, north, 0.0))
        s.xs[1, 1, at, :] = s.xs[1, 1, at, :] - extra
        here = jnp.where(first_lane, s.field[0, at8, :], s.field[1, at8, :])
        curvature = curvature - eights(here * extra)
    send_phase1(1, 1)
    s.part[0, 1] = curvature
    reduce_send(0)

    outer_forward(1, 0)
    reduce_middle(0)
    outer_forward(1, 1)
    relay(1)
    own_spectrum(1)
    wait_mate(1)
    mate_spectrum(1)
    mix(1)
    inner_back(1)
    rz_now, bend = reduce_end(0)
    alpha = rz_now / bend

    def rz_next_part(index, carry):
        at = span(index)
        spectrum = s.spec[0, at, :] - alpha * s.spec[1, at, :]
        mixed = s.mixed[0, at, :] - alpha * s.mixed[1, at, :]
        return carry + eights(spectrum * (mixed * weight_of(at)))

    s.part[1, 0] = lax.fori_loop(0, W // 128, rz_next_part, jnp.zeros((8, L), f32))
    s.part[1, 1] = jnp.zeros((8, L), f32)
    reduce_send(1)

    outer_back(1, 0, False)
    outer_back(1, 1, False)
    reduce_middle(1)

    def first_outputs(start, count):
        at, at8 = pl.ds(start, count), eight_on(start, count)
        a, b = s.xs[0, 0, at, :], s.xs[0, 1, at, :]
        image_a, image_b = s.xs[1, 0, at, :], s.xs[1, 1, at, :]
        rest_a, rest_b = a - alpha * image_a, b - alpha * image_b
        mask = lanes_left(count)
        s.out[1, at, :L] = jnp.where(mask, rest_b, rest_a)
        s.out[1, at, L:] = jnp.where(mask, rest_a, rest_b)
        for k in range(2):
            s.out[0, at, k * L : (k + 1) * L] = alpha * s.field[k, at8, :]

    loop_rows(first_outputs)
    stores = [
        pltpu.make_async_copy(s.out.at[k], ref, s.store.at[k])
        for k, ref in enumerate((solution_ref, residual_ref, direction_ref))
    ]
    stores[0].start()
    stores[1].start()
    rz_next, _ = reduce_end(1)
    beta = rz_next / rz_now
    wait_back(1, 0, False)
    wait_back(1, 1, False)

    def last_output(start, count):
        at, at8 = pl.ds(start, count), eight_on(start, count)
        for k, value in enumerate(fields_of(1, at, count)):
            first = s.field[k, at8, :]
            second = first - alpha * (s.wet[k, at8, :] * value)
            s.out[2, at, k * L : (k + 1) * L] = second + beta * first

    loop_rows(last_output)
    stores[2].start()
    for make, when in pending:
        if when is None:
            make().wait_send()
        else:
            pl.when(when)(functools.partial(lambda make: make().wait_send(), make))
    for store in stores:
        store.wait()


def local(
    surface_forcing,
    ocean_mask,
    self_coupling,
    east_coupling,
    north_coupling,
    zonal_weight,
    aligned_inverse,
    staggered_inverse,
):
    groups, bands = lax.axis_size("lon"), lax.axis_size("lat")
    length, columns = surface_forcing.shape
    block = aligned_inverse.shape[1]
    assert columns == 2 * block and block == 128 and groups % 4 == 0
    chunk = -(-length // (8 * groups)) * 8
    padded = groups * chunk
    while 2 * padded % 128:
        chunk, padded = chunk + 8, padded + 8 * groups
    plan = Plan(groups, bands, length, columns, block, (chunk, padded))
    assert plan.rows <= 1024
    matrix, waves = inner_tables(groups, length, padded)
    lanes = np.repeat(waves[:, :, None], block, axis=2)
    scratch = plan.scratch()
    anywhere = pl.BlockSpec(memory_space=pl.ANY)
    shape = jax.ShapeDtypeStruct((length, columns), jnp.float32)
    return pl.pallas_call(
        functools.partial(kernel, plan, tuple(scratch)),
        out_shape=(shape, shape, shape),
        in_specs=[anywhere] * 10,
        out_specs=(anywhere,) * 3,
        scratch_shapes=list(scratch.values()),
        compiler_params=pltpu.CompilerParams(
            collective_id=0, has_side_effects=True, vmem_limit_bytes=60 * 2**20
        ),
        name="step",
    )(
        surface_forcing, ocean_mask, self_coupling, east_coupling, north_coupling,
        zonal_weight[None, :], aligned_inverse, staggered_inverse,
        jnp.asarray(matrix), jnp.asarray(lanes),
    )


def solution(mesh):
    grid = P("lon", "lat")
    stack = P("lat", None, None)
    return jax.shard_map(
        local,
        mesh=mesh,
        in_specs=(grid, grid, grid, grid, grid, P("lat"), stack, stack),
        out_specs=(grid, grid, grid),
        check_vma=False,
    )
```

```python
import functools

import jax
import jax.numpy as jnp
import numpy as np
from jax import lax
from jax.experimental import pallas as pl
from jax.experimental.pallas import tpu as pltpu
from jax.sharding import PartitionSpec as P

MESH = pl.DeviceIdType.MESH
TILE = 1152


def outer_table(groups):
    table = np.zeros((groups, groups))
    place = np.arange(groups)
    table[0] = 1.0
    table[1] = np.where(place % 2 == 0, 1.0, -1.0)
    for mode in range(1, groups // 2):
        turn = 2.0 * np.pi * (mode * place % groups) / groups
        table[2 * mode] = np.cos(turn)
        table[2 * mode + 1] = -np.sin(turn)
    table[np.abs(table) < 1e-12] = 0.0
    return table


def inner_tables(groups, length, padded):
    total = groups * length
    pairs = groups // 2
    matrix = np.zeros((pairs, 2 * padded, 2 * padded))
    waves = np.zeros((pairs, 2 * padded))
    cell = np.arange(length)

    def turns(modes):
        return 2.0 * np.pi * (modes[:, None] * cell[None, :] % total) / total

    def note(pair, start, modes):
        stop = start + len(modes)
        waves[pair, start:stop] = 2.0 - 2.0 * np.cos(2.0 * np.pi * modes / total)

    for part, (first, real_count) in enumerate(((0, length // 2 + 1), (groups // 2, (length + 1) // 2))):
        skipped = 1 if part == 0 else 0
        real = first + groups * np.arange(real_count)
        imag = first + groups * (skipped + np.arange(length - real_count))
        row = part * padded
        columns = slice(part * padded, part * padded + length)
        matrix[0, row : row + real_count, columns] = np.cos(turns(real))
        matrix[0, row + real_count : row + length, columns] = -np.sin(turns(imag))
        note(0, row, real)
        note(0, row + real_count, imag)
    for pair in range(1, pairs):
        modes = pair + groups * np.arange(length)
        angle = turns(modes)
        low, high = slice(0, length), slice(padded, padded + length)
        matrix[pair, low, low] = np.cos(angle)
        matrix[pair, low, high] = np.sin(angle)
        matrix[pair, high, low] = -np.sin(angle)
        matrix[pair, high, high] = np.cos(angle)
        note(pair, 0, modes)
        note(pair, padded, modes)
    single = matrix.astype(np.float32)
    leading = single.astype(jnp.bfloat16)
    rest = (matrix - leading.astype(np.float64)).astype(jnp.bfloat16)
    return np.stack([leading, rest], axis=1), waves.astype(np.float32)


def parted(value):
    leading = value.astype(jnp.bfloat16)
    return leading, (value - leading.astype(jnp.float32)).astype(jnp.bfloat16)


def dot(left, right):
    return jnp.dot(left, right, preferred_element_type=jnp.float32)


def weighted(values, factors):
    total = None
    for value, factor in zip(values, factors):
        if factor == 0.0:
            continue
        term = value if factor == 1.0 else value * np.float32(factor)
        total = term if total is None else total + term
    return total


class Plan:
    def __init__(self, groups, bands, length, columns, block, width_of):
        self.groups, self.bands, self.length = groups, bands, length
        self.pairs = groups // 2
        self.columns, self.block = columns, block
        self.chunk, self.padded = width_of
        self.width = 2 * self.padded
        self.rows = max(-(-length // 128) * 128, -(-self.padded // 128) * 128)
        self.tile = next(t for t in (TILE, 384, 256, 128) if self.width % t == 0)
        self.table = outer_table(groups)

    def scratch(self):
        f32, bf16 = jnp.float32, jnp.bfloat16
        G, NP, C, PD, W, R, L = (
            self.groups, self.pairs, self.chunk, self.padded, self.width, self.rows, self.block
        )
        vmem, dma = pltpu.VMEM, pltpu.SemaphoreType.DMA
        return {
            "forcing": vmem((self.length, 2 * L), f32),
            "mask": vmem((self.length, 2 * L), jnp.int32),
            "selfc": vmem((self.length, 2 * L), f32),
            "eastc": vmem((self.length, 2 * L), f32),
            "northc": vmem((self.length, 2 * L), f32),
            "zonal": vmem((1, 2 * L), f32),
            "zonal_in": vmem((2, 1, 2 * L), f32),
            "aligned": vmem((2, L, L), f32),
            "staggered": vmem((2, L, L), f32),
            "carried": vmem((L, L), f32),
            "matrix": vmem((2, W, W), bf16),
            "turned": vmem((2, W, W), bf16),
            "wave": vmem((W, L), f32),
            "wet": vmem((2, R + 16, L), f32),
            "east_wet": vmem((2, R, L), f32),
            "east": vmem((2, R + 16, L), f32),
            "north": vmem((2, R, L), f32),
            "south": vmem((2, R, L), f32),
            "diag": vmem((2, R, L), f32),
            "field": vmem((2, R + 16, L), f32),
            "row_in": vmem((3, 2, 8, L), f32),
            "row_out": vmem((3, 2, 8, L), f32),
            "edge_out": vmem((2, 2, 8, L), f32),
            "edge_in": vmem((2, 2, 8, L), f32),
            "scale": vmem((3, W, L), f32),
            "scale_out": vmem((W, L), f32),
            "gain": vmem((3, L, 2 * L), bf16),
            "xs": vmem((2, 2, R, L), f32),
            "got1": vmem((2, 2, G, C, L), f32),
            "send2": vmem((2, NP, 2, 2, C, L), f32),
            "cells": vmem((2, 3, 2, PD, L), f32),
            "zs": vmem((2, 2, PD, L), f32),
            "zgot": vmem((2, 2, PD, L), f32),
            "spec": vmem((2, W, L), f32),
            "mixed": vmem((2, W, L), f32),
            "send3": vmem((2, 2, PD, L), f32),
            "got3": vmem((2, G, 2, C, L), f32),
            "send4": vmem((2, G, 2, C, L), f32),
            "got4": vmem((2, 2, R, L), f32),
            "ew": vmem((2, 2, 8, L), f32),
            "part": vmem((2, 2, 8, L), f32),
            "red1": vmem((2, G, 2, 8, L), f32),
            "middle": vmem((2, 2, 8, L), f32),
            "red2": vmem((2, self.bands, 2, 8, L), f32),
            "out": vmem((3, self.length, 2 * L), f32),
            "store": dma((3,)),
            "load": dma((10,)),
            "s1": dma((2, 2)),
            "r1": dma((2, 2)),
            "s2": dma((2,)),
            "r2": dma((2, NP)),
            "sm": dma((2,)),
            "rm": dma((2,)),
            "sz": dma((2, 2)),
            "rz": dma((2, 2)),
            "s3": dma((2,)),
            "r3": dma((2, 2)),
            "s4": dma((2, 2)),
            "r4": dma((2, 2)),
            "sw": dma((2,)),
            "rw": dma((2,)),
            "srow": dma,
            "rrow": dma,
            "sedge": dma((2, 2)),
            "redge": dma((2, 2)),
            "szon": dma((2,)),
            "rzon": dma((2,)),
            "sstag": dma,
            "rstag": dma,
            "sa": dma((2,)),
            "ra": dma((2,)),
            "sb": dma((2,)),
            "rb": dma((2,)),
        }


class Refs:
    pass


def kernel(plan, names, *refs):
    (forcing_ref, mask_ref, self_ref, east_ref, north_ref, zonal_ref, aligned_ref, staggered_ref,
     matrix_ref, wave_ref, solution_ref, residual_ref, direction_ref) = refs[:13]
    s = Refs()
    for name, ref in zip(names, refs[13:]):
        setattr(s, name, ref)
    G, NP, C, PD, W, R, L = (
        plan.groups, plan.pairs, plan.chunk, plan.padded, plan.width, plan.rows, plan.block
    )
    bands, length, tile, table = plan.bands, plan.length, plan.tile, plan.table
    half = L // 2
    total = G * length
    f32 = jnp.float32
    band = lax.axis_index("lat")
    me = lax.axis_index("lon")
    pair, core = me // 2, me % 2
    mate = me + 1 - 2 * core
    has_up, has_down = band < bands - 1, band > 0
    sends_up, sends_down = (core == 1) & has_up, (core == 1) & has_down
    STEPS = [(d, e) for d in range(1, NP) for e in (0, 1)] + [(0, 1)]
    last_chunk = (length - 1) // C
    last_tile = (length - 1) // 8 * 8
    last_row = (length - 1) % 8

    def to_dev(d, e):
        return 2 * ((pair + d) % NP) + (core + e) % 2

    def from_dev(d, e):
        return 2 * ((pair - d + NP) % NP) + (core + e) % 2

    def remote(src, dst, send, recv, device):
        return pltpu.make_async_remote_copy(
            src_ref=src, dst_ref=dst, send_sem=send, recv_sem=recv,
            device_id=device, device_id_type=MESH,
        )

    pending = []

    def launch(make, when=None):
        if when is None:
            make().start()
        else:
            pl.when(when)(lambda: make().start())

    def recv_all(ref, sem, when=None):
        def wait():
            remote(ref, ref, sem, sem, (band, mate)).wait_recv()
        wait() if when is None else pl.when(when)(wait)

    def sent(ref, sem, when=None):
        pending.append((ref, sem, when))

    def drain():
        for ref, sem, when in pending:
            def wait(ref=ref, sem=sem):
                remote(ref, ref, sem, sem, (band, mate)).wait_send()
            wait() if when is None else pl.when(when)(wait)
        pending.clear()

    def chunks(t, count):
        return s.got3.at[t, pl.ds(0, count)]

    def rows(index):
        return pl.ds(pl.multiple_of(index * C, 8), C)

    def span(index, size=128):
        return pl.ds(pl.multiple_of(index * size, size), size)

    def loop(count, body):
        def step(index, carry):
            body(index)
            return carry
        lax.fori_loop(0, count, step, 0)

    def eight_on(start, count):
        return pl.ds(start + 8 if isinstance(start, int) else pl.multiple_of(start + 8, 8), count)

    def loop_rows(body):
        full = length // 128
        loop(full, lambda index: body(pl.multiple_of(index * 128, 128), 128))
        if length % 128:
            body(full * 128, length % 128)

    def lanes_left(count):
        return lax.broadcasted_iota(jnp.int32, (count, L), 1) < half

    def groups_of(t0, t1):
        mask = lanes_left(t0.shape[0])
        return jnp.where(mask, t1, t0), jnp.where(mask, t0, t1)

    loads = []
    for index, (src, dst) in enumerate((
        (forcing_ref, s.forcing),
        (mask_ref, s.mask),
        (matrix_ref.at[pair], s.matrix),
        (wave_ref.at[pair], s.wave),
        (self_ref, s.selfc),
        (east_ref, s.eastc),
        (north_ref, s.northc),
        (zonal_ref, s.zonal),
        (aligned_ref, s.aligned),
        (staggered_ref, s.staggered),
    )):
        loads.append(pltpu.make_async_copy(src, dst, s.load.at[index]))
    loads[0].start()
    loads[1].start()

    barrier = pltpu.get_barrier_semaphore()
    for d, e in STEPS:
        pl.semaphore_signal(barrier, inc=1, device_id=(band, to_dev(d, e)), device_id_type=MESH)
    for side, has in ((band + 1, has_up), (band - 1, has_down)):
        @pl.when(has)
        def _(side=side):
            pl.semaphore_signal(barrier, inc=1, device_id=(side, me), device_id_type=MESH)

    loads[0].wait()
    loads[1].wait()
    for load in loads[2:]:
        load.start()
    s.xs[0, :, length:R, :] = jnp.zeros((2, R - length, L), f32)
    s.wet[:, 8 + length : 16 + R, :] = jnp.zeros((2, R + 8 - length, L), f32)
    s.field[:, 8 + R : 16 + R, :] = jnp.zeros((2, 8, L), f32)

    def make_rhs(start, count):
        at = pl.ds(start, count)
        wet = s.mask[at, :].astype(f32)
        rhs = wet * s.forcing[at, :]
        a, b = groups_of(rhs[:, :L], rhs[:, L:])
        s.xs[0, 0, at, :] = a
        s.xs[0, 1, at, :] = b
        at8 = eight_on(start, count)
        s.wet[0, at8, :] = wet[:, :L]
        s.wet[1, at8, :] = wet[:, L:]

    loop_rows(make_rhs)
    pl.semaphore_wait(barrier, G - 1 + has_up.astype(jnp.int32) + has_down.astype(jnp.int32))

    def send_phase1(t, g):
        for d, e in STEPS:
            to = to_dev(d, e)
            remote(s.xs.at[t, g, rows(to)], s.got1.at[t, g, me],
                   s.s1.at[t, g], s.r1.at[t, g], (band, to)).start()
        sent(s.got1.at[t, g, pl.ds(0, G - 1)], s.s1.at[t, g])
        s.got1[t, g, me] = s.xs[t, g, rows(me), :]

    def outer_forward(t, g):
        recv_all(s.got1.at[t, g, pl.ds(0, G - 1)], s.r1.at[t, g])

        def step(index):
            at = span(index, 8)
            values = [s.got1[t, g, place, at, :] for place in range(G)]
            for row in range(G):
                s.send2[t, row // 2, g, row % 2, at, :] = weighted(values, table[row])

        loop(C // 8, step)
        for d in list(range(1, NP)) + [0]:
            def make(d=d):
                to = (pair + d) % NP
                return remote(
                    s.send2.at[t, to, g], s.cells.at[t, 0, :, rows(me), :],
                    s.s2.at[t], s.r2.at[t, d], (band, 2 * to + g))
            launch(make, None if d else core != g)

        @pl.when(core == g)
        def _():
            s.cells[t, 0, :, rows(me), :] = s.send2[t, pair, g]

    def pair_rows(d):
        return pl.ds(pl.multiple_of((pair - d + NP) % NP * (2 * C), 16), 2 * C)

    def relay(t, steps):
        for d in steps:
            recv_all(chunks(t, 2 if d else 1), s.r2.at[t, d])
            at = pair_rows(d)
            remote(s.cells.at[t, 0, :, at, :], s.cells.at[t, 1, :, at, :],
                   s.sm.at[t], s.rm.at[t], (band, mate)).start()

            @pl.when(core == 1)
            def _():
                low, high = s.cells[t, 0, 0, at, :], s.cells[t, 0, 1, at, :]
                mask = lanes_left(2 * C)
                s.zs[t, 0, at, :] = jnp.where(mask, low, pltpu.roll(high, half, 1))
                s.zs[t, 1, at, :] = jnp.where(mask, pltpu.roll(low, half, 1), high)

            for way, has in ((0, sends_down), (1, sends_up)):
                def make(way=way):
                    return remote(s.zs.at[t, way, at, :], s.zgot.at[t, way, at, :],
                                  s.sz.at[t, way], s.rz.at[t, way], (band - 1 + 2 * way, me))
                launch(make, has)

    def wait_mate(t):
        recv_all(s.cells.at[t, 1], s.rm.at[t])

    def wait_across(t):
        for way, has in ((0, has_up), (1, has_down)):
            recv_all(s.zgot.at[t, way], s.rz.at[t, way], has)

        def step(index):
            size = G // 2 * C
            at = pl.ds(pl.multiple_of(index * size, 8), size)
            above, below = s.zgot[t, 0, at, :], s.zgot[t, 1, at, :]
            mask = lanes_left(size)
            s.cells[t, 2, 0, at, :] = jnp.where(mask, above, pltpu.roll(below, half, 1))
            s.cells[t, 2, 1, at, :] = jnp.where(mask, pltpu.roll(above, half, 1), below)

        loop(2, step)

    def transform(t, which, start):
        hi, lo = parted(s.cells[t, which].reshape(W, L))
        both = jnp.concatenate([hi, lo], axis=1)

        def step(index):
            at = span(index, tile)
            wide = dot(s.matrix[0, at, :], both)
            value = wide[:, :L] + (wide[:, L:] + dot(s.matrix[1, at, :], hi))
            value = value * s.scale[which, at, :]

            @pl.when(which == 0)
            def _():
                s.spec[t, at, :] = value

            high, low = parted(value)
            wide = dot(high, s.gain[which])
            mixed = wide[:, :L] + (wide[:, L:] + dot(low, s.gain[which, :, :L]))
            if not start:
                mixed = mixed + s.mixed[t, at, :]
            s.mixed[t, at, :] = mixed

        loop(W // tile, step)

    NEAR, FAR = [0], list(range(1, NP))

    def inner_forward(t, late):
        early = core != late

        @pl.when(early)
        def _():
            relay(t, NEAR + FAR)

        @pl.when(jnp.logical_not(early))
        def _():
            relay(t, NEAR)
            wait_mate(t)

        sent(chunks(t, G - 1), s.s2.at[t])
        sent(s.cells.at[t, 1], s.sm.at[t])
        sent(s.zgot.at[t, 0], s.sz.at[t, 0], sends_down)
        sent(s.zgot.at[t, 1], s.sz.at[t, 1], sends_up)
        transform(t, jnp.where(early, 0, 1), True)

        @pl.when(jnp.logical_not(early))
        def _():
            relay(t, FAR)

        def outer_part():
            @pl.when(core == 1)
            def _():
                wait_across(t)
                transform(t, 2, False)

        if late == 0:
            outer_part()

        @pl.when(early)
        def _():
            wait_mate(t)

        transform(t, jnp.where(early, 1, 0), False)
        if late == 1:
            outer_part()

    def inner_back(t):
        hi, lo = parted(s.mixed[t] * s.scale_out[...])
        both = jnp.concatenate([hi, lo], axis=1)
        size = G // 2 * C
        first = 1 - me // (G // 2)
        for turn in range(2):
            side = first if turn == 0 else 1 - first
            for part in range(2):
                at = pl.ds(pl.multiple_of(part * PD + side * size, 16), size)
                wide = dot(s.turned[0, at, :], both)
                s.send3[t, part, pl.ds(pl.multiple_of(side * size, 8), size), :] = (
                    wide[:, :L] + (wide[:, L:] + dot(s.turned[1, at, :], hi)))
            for d, e in STEPS:
                def make(d=d, e=e):
                    to = to_dev(d, e)
                    return remote(s.send3.at[t, :, rows(to), :], s.got3.at[t, me],
                                  s.s3.at[t], s.r3.at[t, core], (band, to))
                launch(make, to_dev(d, e) // (G // 2) == side)
        sent(chunks(t, G - 1), s.s3.at[t])
        s.got3[t, me] = s.send3[t, :, rows(me), :]

    def outer_back(t, g, edges):
        recv_all(chunks(t, NP), s.r3.at[t, g], core != g)
        recv_all(chunks(t, NP - 1), s.r3.at[t, g], core == g)

        def step(index):
            at = span(index, 8)
            values = [s.got3[t, 2 * (row // 2) + g, row % 2, at, :] for row in range(G)]
            for place in range(G):
                s.send4[t, place, g, at, :] = weighted(values, table[:, place])

        loop(C // 8, step)
        for d, e in STEPS:
            to = to_dev(d, e)
            remote(s.send4.at[t, to, g], s.got4.at[t, g, rows(me), :],
                   s.s4.at[t, g], s.r4.at[t, g], (band, to)).start()
        sent(s.got1.at[t, g, pl.ds(0, G - 1)], s.s4.at[t, g])
        s.got4[t, g, rows(me), :] = s.send4[t, me, g]
        if not edges:
            return
        for way, (owner, shift, at) in enumerate((
            (0, 1, 0), (last_chunk, G - 1, (length - 1) % C // 8 * 8))):
            @pl.when(me == owner)
            def _(way=way, shift=shift, at=at):
                for d, e in STEPS:
                    to = to_dev(d, e)
                    remote(s.send4.at[t, (to + shift) % G, g, pl.ds(at, 8), :], s.ew.at[way, g],
                           s.sw.at[way], s.rw.at[way], (band, to)).start()
                s.ew[way, g] = s.send4[t, (me + shift) % G, g, pl.ds(at, 8), :]

            if g == 1:
                sent(s.red1.at[0, pl.ds(0, G - 1)], s.sw.at[way], me == owner)

    def wait_back(t, g):
        recv_all(s.got1.at[t, g, pl.ds(0, G - 1)], s.r4.at[t, g])

    def wait_rows():
        for way, owner in enumerate((0, last_chunk)):
            recv_all(s.ew.at[way], s.rw.at[way], me != owner)

    def send_edges(i):
        for way, (side, has) in enumerate(((band - 1, has_down), (band + 1, has_up))):
            def make(way=way, side=side):
                return remote(s.edge_out.at[i, way], s.edge_in.at[i, way],
                              s.sedge.at[i, way], s.redge.at[i, way], (side, me))
            launch(make, has)
            sent(s.edge_out.at[i, way], s.sedge.at[i, way], has)

    def wait_edges(i):
        for way, has in enumerate((has_up, has_down)):
            recv_all(s.edge_in.at[i, way], s.redge.at[i, way], has)

    def column_of(i, way):
        tile8 = s.edge_in[i, way]
        return jnp.concatenate([tile8, jnp.zeros((L - 8, L), f32)], axis=0).T

    def reduce_send(i):
        for d, e in STEPS:
            remote(s.part.at[i], s.red1.at[i, me], s.sa.at[i], s.ra.at[i],
                   (band, to_dev(d, e))).start()
        sent(s.red1.at[i, pl.ds(0, G - 1)], s.sa.at[i])
        s.red1[i, me] = s.part[i]

    def reduce_middle(i):
        recv_all(s.red1.at[i, pl.ds(0, G - 1)], s.ra.at[i])
        value = s.red1[i, 0]
        for place in range(1, G):
            value = value + s.red1[i, place]
        s.middle[i] = value
        s.red2[i, band] = value
        for step in range(1, bands):
            remote(s.middle.at[i], s.red2.at[i, band], s.sb.at[i], s.rb.at[i],
                   ((band + step) % bands, me)).start()
        sent(s.red2.at[i, pl.ds(0, bands - 1)], s.sb.at[i])

    def reduce_end(i):
        recv_all(s.red2.at[i, pl.ds(0, bands - 1)], s.rb.at[i])
        value = s.red2[i, 0]
        for place in range(1, bands):
            value = value + s.red2[i, place]
        return [jnp.sum(value[k], keepdims=True) for k in range(2)]

    def eights(value):
        return value.reshape(value.shape[0] // 8, 8, L).sum(axis=0)

    def weight_of(at):
        wave = s.wave[at, :]
        edge = (wave == 0.0) | (wave == 4.0)
        return jnp.where(edge, np.float32(1.0 / total), np.float32(2.0 / total))

    send_phase1(0, 1)
    send_phase1(0, 0)

    blocks = R // 128

    def shifted(index, by=8):
        return pl.ds(pl.multiple_of(index * 128 + by, 8), 128)

    for load in loads[4:]:
        load.wait()
    for ref in (s.east_wet, s.north):
        ref[:, length:R, :] = jnp.zeros((2, R - length, L), f32)

    def make_faces(start, count):
        at, at8 = pl.ds(start, count), eight_on(start, count)
        for k in range(2):
            lanes = slice(k * L, (k + 1) * L)
            wet = s.wet[k, at8, :]
            s.east_wet[k, at, :] = s.eastc[at, lanes] * wet
            s.north[k, at, :] = s.northc[at, lanes] * wet

    loop_rows(make_faces)
    west_dev, east_dev = (me + G - 1) % G, (me + 1) % G
    s.row_out[0] = s.wet[:, 8:16, :]
    s.row_out[1] = s.wet[:, 8 + last_tile : 16 + last_tile, :]
    s.row_out[2] = s.east_wet[:, last_tile : last_tile + 8, :]
    for k, device in enumerate((west_dev, east_dev, east_dev)):
        remote(s.row_out.at[k], s.row_in.at[k], s.srow, s.rrow, (band, device)).start()
    sent(s.row_in, s.srow)

    def take_edges(i, low, high, by):
        for b in range(blocks):
            s.edge_out[i, 0, b : b + 1, :] = low[pl.ds(128 * b + by[0], 128), :].T[:1, :]
            s.edge_out[i, 1, b : b + 1, :] = high[pl.ds(128 * b + by[1], 128), :].T[L - 1 :, :]
        if blocks < 8:
            s.edge_out[i, :, blocks:, :] = jnp.zeros((2, 8 - blocks, L), f32)

    take_edges(0, s.wet.at[0], s.north.at[1], (8, 0))
    send_edges(0)
    for way, (side, has) in enumerate(((band - 1, has_down), (band + 1, has_up))):
        def send_zonal(way=way, side=side):
            return remote(
                s.zonal, s.zonal_in.at[way], s.szon.at[way], s.rzon.at[way], (side, me))
        launch(send_zonal, has)
        sent(s.zonal, s.szon.at[way], has)

    def send_stag():
        return remote(s.staggered.at[1], s.carried, s.sstag, s.rstag, (band + 1, me))

    launch(send_stag, has_up)
    sent(s.carried, s.sstag, has_up)
    for way, has in enumerate((has_up, has_down)):
        @pl.when(jnp.logical_not(has))
        def _(way=way):
            for i in range(2):
                s.edge_in[i, way] = jnp.zeros((8, L), f32)
                s.zgot[i, way] = jnp.zeros((PD, L), f32)
            s.zonal_in[way] = jnp.zeros((1, 2 * L), f32)

    @pl.when(jnp.logical_not(has_down))
    def _():
        s.carried[...] = jnp.zeros((L, L), f32)

    loads[2].wait()
    loads[3].wait()

    def turn(index):
        at = span(index)
        for k in range(2):
            s.turned[k, at, :] = s.matrix[k, :, at].T

    loop(W // 128, turn)

    outer_forward(0, 1)
    outer_forward(0, 0)

    for way, has in enumerate((has_up, has_down)):
        recv_all(s.zonal_in.at[way], s.rzon.at[way], has)
    z0, z1 = s.zonal[:, :L], s.zonal[:, L:]
    mask1 = lanes_left(1)
    zone_a, zone_b = jnp.where(mask1, z1, z0), jnp.where(mask1, z0, z1)
    is_low = core == 0
    zones = (
        jnp.where(is_low, zone_a, zone_b),
        jnp.where(is_low, zone_b, zone_a),
        jnp.where(mask1, s.zonal_in[0, :, :L], s.zonal_in[1, :, L:]),
    )

    def make_scale(index):
        at = span(index)
        wave = s.wave[at, :]
        for k, zone in enumerate(zones):
            s.scale[k, at, :] = lax.rsqrt(1.0 + wave * zone)
        s.scale_out[at, :] = s.scale[0, at, :] * weight_of(at)

    loop(W // 128, make_scale)

    recv_all(s.carried, s.rstag, has_down)

    def swapped(value):
        value = jnp.concatenate([value[half:, :], value[:half, :]], axis=0)
        return pltpu.roll(value, half, 1)

    row_top = lax.broadcasted_iota(jnp.int32, (L, L), 0) < half
    col_left = lanes_left(L)
    tl, tr = row_top & col_left, row_top & jnp.logical_not(col_left)
    bl = jnp.logical_not(row_top) & col_left
    br = jnp.logical_not(row_top) & jnp.logical_not(col_left)
    al0, al1 = s.aligned[0], s.aligned[1]
    mid, top, low = swapped(s.staggered[0]), swapped(s.staggered[1]), swapped(s.carried[...])
    zero = jnp.zeros((L, L), f32)

    def pick(*items):
        value = zero
        for where, block in items:
            value = jnp.where(where, block, value)
        return value

    own = jnp.where(
        is_low, mid + pick((tl, al1), (br, al0)), pick((tl, al0 + low), (br, al1 + top)))
    beside = jnp.where(is_low, pick((tr, al0), (bl, al1)), pick((tr, al1), (bl, al0)))
    across = pick((tr, top), (bl, low))
    for k, value in enumerate((own, beside, across)):
        hi, lo = parted(value)
        s.gain[k, :, :L] = hi
        s.gain[k, :, L:] = lo

    inner_forward(0, 0)
    inner_back(0)

    def rz_part(index, carry):
        at = span(index)
        return carry + eights(s.spec[0, at, :] * (s.mixed[0, at, :] * weight_of(at)))

    s.part[0, 0] = lax.fori_loop(0, W // 128, rz_part, jnp.zeros((8, L), f32))

    recv_all(s.row_in, s.rrow)
    wait_edges(0)
    north_col, south_col = column_of(0, 0), column_of(0, 1)
    for k in range(2):
        s.wet[k, 8 + length : 9 + length, :] = s.row_in[0, k, 0:1, :]
        s.east[k, 7:8, :] = s.row_in[2, k, last_row : last_row + 1, :] * s.wet[k, 8:9, :]
    lane = lax.broadcasted_iota(jnp.int32, (128, L), 1)
    first_lane, last_lane = lane == 0, lane == L - 1
    for b in range(blocks):
        at, at8, at9 = pl.ds(128 * b, 128), pl.ds(128 * b + 8, 128), pl.ds(128 * b + 9, 128)
        wet = [s.wet[k, at8, :] for k in range(2)]
        east = [s.east_wet[k, at, :] * s.wet[k, at9, :] for k in range(2)]
        moved = [pltpu.roll(value, L - 1, 1) for value in wet]
        beyond = jnp.broadcast_to(north_col[:, b : b + 1], (128, L))
        north = [
            s.north[0, at, :] * jnp.where(last_lane, moved[1], moved[0]),
            s.north[1, at, :] * jnp.where(last_lane, beyond, moved[1]),
        ]
        moved = [pltpu.roll(value, 1, 1) for value in north]
        beyond = jnp.broadcast_to(south_col[:, b : b + 1], (128, L))
        south = [
            jnp.where(first_lane, beyond * wet[0], moved[0]),
            jnp.where(first_lane, moved[0], moved[1]),
        ]
        for k in range(2):
            s.east[k, at8, :] = east[k]
            s.north[k, at, :] = north[k]
            s.south[k, at, :] = south[k]
    def make_diag(start, count):
        at, at8 = pl.ds(start, count), eight_on(start, count)
        for k in range(2):
            wet = s.wet[k, at8, :]
            own = (1.0 - wet) + wet * s.selfc[at, k * L : (k + 1) * L]
            s.diag[k, at, :] = own + s.diag[k, at, :]

    for b in range(blocks):
        at, at8, at7 = pl.ds(128 * b, 128), pl.ds(128 * b + 8, 128), pl.ds(128 * b + 7, 128)
        for k in range(2):
            s.diag[k, at, :] = (
                (s.east[k, at8, :] + s.east[k, at7, :]) + (s.north[k, at, :] + s.south[k, at, :]))
    s.diag[:, length:R, :] = jnp.zeros((2, R - length, L), f32)
    loop_rows(make_diag)
    if R > PD:
        for t in range(2):
            for g in range(2):
                s.got4[t, g, PD:, :] = jnp.zeros((R - PD, L), f32)

    drain()
    outer_back(0, 0, True)
    outer_back(0, 1, True)
    wait_back(0, 0)
    wait_back(0, 1)
    wait_rows()

    def fields_of(t, at, count):
        a, b = s.got4[t, 0, at, :], s.got4[t, 1, at, :]
        mask = lanes_left(count)
        return jnp.where(mask, b, a), jnp.where(mask, a, b)

    def make_field(index):
        at8 = shifted(index)
        for k, value in enumerate(fields_of(0, span(index), 128)):
            s.field[k, at8, :] = s.wet[k, at8, :] * value

    loop(blocks, make_field)
    take_edges(1, s.field.at[0], s.field.at[1], (8, 8))
    send_edges(1)
    mask1 = lanes_left(1)
    for way, (row, source) in enumerate(((0, 0), (last_row, 1))):
        a, b = s.ew[way, 0, row : row + 1, :], s.ew[way, 1, row : row + 1, :]
        for k, value in enumerate((jnp.where(mask1, b, a), jnp.where(mask1, a, b))):
            at = 8 + length if way == 0 else 7
            s.field[k, at : at + 1, :] = s.row_in[source, k, row : row + 1, :] * value

    curvature = jnp.zeros((8, L), f32)
    for b in range(blocks):
        at, at8 = pl.ds(128 * b, 128), pl.ds(128 * b + 8, 128)
        at7, at9 = pl.ds(128 * b + 7, 128), pl.ds(128 * b + 9, 128)
        here = [s.field[k, at8, :] for k in range(2)]
        up = [pltpu.roll(value, L - 1, 1) for value in here]
        down = [pltpu.roll(value, 1, 1) for value in here]
        up = [jnp.where(last_lane, up[1], up[0]), jnp.where(last_lane, 0.0, up[1])]
        down = [jnp.where(first_lane, 0.0, down[0]), jnp.where(first_lane, down[0], down[1])]
        image = []
        for k in range(2):
            value = s.diag[k, at, :] * here[k]
            value = value - s.east[k, at8, :] * s.field[k, at9, :]
            value = value - s.east[k, at7, :] * s.field[k, at7, :]
            value = value - s.north[k, at, :] * up[k]
            value = value - s.south[k, at, :] * down[k]
            if 128 * (b + 1) > length:
                row = lax.broadcasted_iota(jnp.int32, (128, L), 0)
                value = jnp.where(row < length - 128 * b, value, 0.0)
            image.append(value)
            curvature = curvature + eights(here[k] * image[k])
        s.xs[1, 0, at, :], s.xs[1, 1, at, :] = groups_of(*image)

    send_phase1(1, 0)
    wait_edges(1)
    north_col, south_col = column_of(1, 0), column_of(1, 1)
    for b in range(blocks):
        at, at8 = pl.ds(128 * b, 128), pl.ds(128 * b + 8, 128)
        south = s.south[0, at, :] * jnp.broadcast_to(south_col[:, b : b + 1], (128, L))
        north = s.north[1, at, :] * jnp.broadcast_to(north_col[:, b : b + 1], (128, L))
        extra = jnp.where(first_lane, south, jnp.where(last_lane, north, 0.0))
        s.xs[1, 1, at, :] = s.xs[1, 1, at, :] - extra
        here = jnp.where(first_lane, s.field[0, at8, :], s.field[1, at8, :])
        curvature = curvature - eights(here * extra)
    send_phase1(1, 1)
    s.part[0, 1] = curvature
    reduce_send(0)
    drain()

    outer_forward(1, 0)
    outer_forward(1, 1)
    reduce_middle(0)
    inner_forward(1, 1)
    inner_back(1)
    rz_now, bend = reduce_end(0)
    alpha = rz_now / bend

    def rz_next_part(index, carry):
        at = span(index)
        spectrum = s.spec[0, at, :] - alpha * s.spec[1, at, :]
        mixed = s.mixed[0, at, :] - alpha * s.mixed[1, at, :]
        return carry + eights(spectrum * (mixed * weight_of(at)))

    s.part[1, 0] = lax.fori_loop(0, W // 128, rz_next_part, jnp.zeros((8, L), f32))
    s.part[1, 1] = jnp.zeros((8, L), f32)
    reduce_send(1)

    drain()
    outer_back(1, 0, False)
    reduce_middle(1)
    outer_back(1, 1, False)

    def first_outputs(start, count):
        at, at8 = pl.ds(start, count), eight_on(start, count)
        mask = lanes_left(count)
        rest = [s.xs[0, g, at, :] - alpha * s.xs[1, g, at, :] for g in range(2)]
        s.out[1, at, :L] = jnp.where(mask, rest[1], rest[0])
        s.out[1, at, L:] = jnp.where(mask, rest[0], rest[1])
        for k in range(2):
            s.out[0, at, k * L : (k + 1) * L] = alpha * s.field[k, at8, :]

    loop_rows(first_outputs)
    stores = [
        pltpu.make_async_copy(s.out.at[k], ref, s.store.at[k])
        for k, ref in enumerate((solution_ref, residual_ref, direction_ref))
    ]
    stores[0].start()
    stores[1].start()
    rz_next, _ = reduce_end(1)
    beta = rz_next / rz_now
    wait_back(1, 0)
    drain()
    wait_back(1, 1)

    def last_output(start, count):
        at, at8 = pl.ds(start, count), eight_on(start, count)
        for k, value in enumerate(fields_of(1, at, count)):
            first = s.field[k, at8, :]
            second = first - alpha * (s.wet[k, at8, :] * value)
            s.out[2, at, k * L : (k + 1) * L] = second + beta * first

    loop_rows(last_output)
    stores[2].start()
    for store in stores:
        store.wait()
    drain()


def finish_kernel(*refs):
    ins, outs, held, arrived, left = refs[:3], refs[3:6], refs[6], refs[7], refs[8]
    gets = [pltpu.make_async_copy(ref, held.at[k], arrived.at[k]) for k, ref in enumerate(ins)]
    puts = [pltpu.make_async_copy(held.at[k], ref, left.at[k]) for k, ref in enumerate(outs)]
    for get in gets:
        get.start()
    for get, put in zip(gets, puts):
        get.wait()
        put.start()
    for put in puts:
        put.wait()


def local(
    surface_forcing,
    ocean_mask,
    self_coupling,
    east_coupling,
    north_coupling,
    zonal_weight,
    aligned_inverse,
    staggered_inverse,
):
    groups, bands = lax.axis_size("lon"), lax.axis_size("lat")
    length, columns = surface_forcing.shape
    block = aligned_inverse.shape[1]
    assert columns == 2 * block and block == 128 and groups % 4 == 0
    chunk = -(-length // (8 * groups)) * 8
    padded = groups * chunk
    while 2 * padded % 128:
        chunk, padded = chunk + 8, padded + 8 * groups
    plan = Plan(groups, bands, length, columns, block, (chunk, padded))
    assert plan.rows <= 1024
    matrix, waves = inner_tables(groups, length, padded)
    lanes = np.repeat(waves[:, :, None], block, axis=2)
    scratch = plan.scratch()
    anywhere = pl.BlockSpec(memory_space=pl.ANY)
    shape = jax.ShapeDtypeStruct((length, columns), jnp.float32)
    outs = pl.pallas_call(
        functools.partial(kernel, plan, tuple(scratch)),
        out_shape=(shape,) * 3,
        in_specs=[anywhere] * 10,
        out_specs=(anywhere,) * 3,
        scratch_shapes=list(scratch.values()),
        compiler_params=pltpu.CompilerParams(
            collective_id=0, has_side_effects=True, vmem_limit_bytes=61 * 2**20
        ),
        name="step",
    )(
        surface_forcing, ocean_mask, self_coupling, east_coupling, north_coupling,
        zonal_weight[None, :], aligned_inverse, staggered_inverse,
        jnp.asarray(matrix), jnp.asarray(lanes),
    )
    return pl.pallas_call(
        finish_kernel,
        out_shape=(shape,) * 3,
        in_specs=[anywhere] * 3,
        out_specs=(anywhere,) * 3,
        scratch_shapes=[
            pltpu.VMEM((3, length, columns), jnp.float32),
            pltpu.SemaphoreType.DMA((3,)),
            pltpu.SemaphoreType.DMA((3,)),
        ],
        name="finish",
    )(*outs)


def solution(mesh):
    grid = P("lon", "lat")
    stack = P("lat", None, None)
    return jax.shard_map(
        local,
        mesh=mesh,
        in_specs=(grid, grid, grid, grid, grid, P("lat"), stack, stack),
        out_specs=(grid, grid, grid),
        check_vma=False,
    )
```

```python
import functools

import jax
import jax.numpy as jnp
import numpy as np
from jax import lax
from jax.experimental import pallas as pl
from jax.experimental.pallas import tpu as pltpu
from jax.sharding import PartitionSpec as P

MESH = pl.DeviceIdType.MESH
TILE = 576


def outer_table(groups):
    table = np.zeros((groups, groups))
    place = np.arange(groups)
    table[0] = 1.0
    table[1] = np.where(place % 2 == 0, 1.0, -1.0)
    for mode in range(1, groups // 2):
        turn = 2.0 * np.pi * (mode * place % groups) / groups
        table[2 * mode] = np.cos(turn)
        table[2 * mode + 1] = -np.sin(turn)
    table[np.abs(table) < 1e-12] = 0.0
    return table


def inner_tables(groups, length, padded):
    total = groups * length
    pairs = groups // 2
    matrix = np.zeros((pairs, 2 * padded, 2 * padded))
    waves = np.zeros((pairs, 2 * padded))
    cell = np.arange(length)

    def turns(modes):
        return 2.0 * np.pi * (modes[:, None] * cell[None, :] % total) / total

    def note(pair, start, modes):
        stop = start + len(modes)
        waves[pair, start:stop] = 2.0 - 2.0 * np.cos(2.0 * np.pi * modes / total)

    for part, (first, real_count) in enumerate(((0, length // 2 + 1), (groups // 2, (length + 1) // 2))):
        skipped = 1 if part == 0 else 0
        real = first + groups * np.arange(real_count)
        imag = first + groups * (skipped + np.arange(length - real_count))
        row = part * padded
        columns = slice(part * padded, part * padded + length)
        matrix[0, row : row + real_count, columns] = np.cos(turns(real))
        matrix[0, row + real_count : row + length, columns] = -np.sin(turns(imag))
        note(0, row, real)
        note(0, row + real_count, imag)
    for pair in range(1, pairs):
        modes = pair + groups * np.arange(length)
        angle = turns(modes)
        low, high = slice(0, length), slice(padded, padded + length)
        matrix[pair, low, low] = np.cos(angle)
        matrix[pair, low, high] = np.sin(angle)
        matrix[pair, high, low] = -np.sin(angle)
        matrix[pair, high, high] = np.cos(angle)
        note(pair, 0, modes)
        note(pair, padded, modes)
    single = matrix.astype(np.float32)
    leading = single.astype(jnp.bfloat16)
    rest = (matrix - leading.astype(np.float64)).astype(jnp.bfloat16)
    return np.stack([leading, rest], axis=1), waves.astype(np.float32)


def parted(value):
    leading = value.astype(jnp.bfloat16)
    return leading, (value - leading.astype(jnp.float32)).astype(jnp.bfloat16)


def dot(left, right):
    return jnp.dot(left, right, preferred_element_type=jnp.float32)


def weighted(values, factors):
    total = None
    for value, factor in zip(values, factors):
        if factor == 0.0:
            continue
        term = value if factor == 1.0 else value * np.float32(factor)
        total = term if total is None else total + term
    return total


class Plan:
    def __init__(self, groups, bands, length, columns, block, width_of):
        self.groups, self.bands, self.length = groups, bands, length
        self.pairs = groups // 2
        self.columns, self.block = columns, block
        self.chunk, self.padded = width_of
        self.width = 2 * self.padded
        self.rows = max(-(-length // 128) * 128, -(-self.padded // 128) * 128)
        self.tile = next(t for t in (TILE, 384, 256, 128) if self.width % t == 0)
        self.table = outer_table(groups)
        tiles = -(-(-(-length // 8)) // self.pairs)
        self.pair_size = 8 * tiles
        self.sizes = (-(-tiles // 2) * 8, tiles // 2 * 8)
        assert self.sizes[0] <= self.chunk and self.sizes[1] > 0
        self.pieces = []
        for size in self.sizes:
            cut = -(-size // 16) * 8
            self.pieces.append([(0, cut)] + ([(cut, size - cut)] if cut < size else []))

    def scratch(self):
        f32, bf16 = jnp.float32, jnp.bfloat16
        G, NP, C, PD, W, R, L = (
            self.groups, self.pairs, self.chunk, self.padded, self.width, self.rows, self.block
        )
        vmem, dma = pltpu.VMEM, pltpu.SemaphoreType.DMA
        return {
            "forcing": vmem((self.length, 2 * L), f32),
            "mask": vmem((self.length, 2 * L), jnp.int32),
            "selfc": vmem((self.length, 2 * L), f32),
            "eastc": vmem((self.length, 2 * L), f32),
            "northc": vmem((self.length, 2 * L), f32),
            "zonal": vmem((1, 2 * L), f32),
            "zonal_in": vmem((2, 1, 2 * L), f32),
            "aligned": vmem((2, L, L), f32),
            "staggered": vmem((2, L, L), f32),
            "carried": vmem((L, L), f32),
            "matrix": vmem((2, W, W), bf16),
            "turned": vmem((2, W, W), bf16),
            "wave": vmem((W, L), f32),
            "wet": vmem((2, R + 16, L), f32),
            "east_wet": vmem((2, R, L), f32),
            "east": vmem((2, R + 16, L), f32),
            "north": vmem((2, R, L), f32),
            "south": vmem((2, R, L), f32),
            "diag": vmem((2, R, L), f32),
            "field": vmem((2, R + 16, L), f32),
            "row_in": vmem((3, 2, 8, L), f32),
            "row_out": vmem((3, 2, 8, L), f32),
            "edge_out": vmem((2, 2, 8, L), f32),
            "edge_in": vmem((2, 2, 8, L), f32),
            "scale": vmem((2, W, L), f32),
            "scale_out": vmem((W, L), f32),
            "gain": vmem((3 * L, 2 * L), bf16),
            "xs": vmem((2, 2, R, L), f32),
            "got1": vmem((2, 2, G, C, L), f32),
            "send2": vmem((2, NP, 2, 2, C, L), f32),
            "cells": vmem((2, 2, 2, PD, L), f32),
            "zs": vmem((2, 2, PD, L), f32),
            "zgot": vmem((2, 2, PD, L), f32),
            "spec": vmem((2, W, L), f32),
            "spec_mate": vmem((2, W, L), f32),
            "mixed": vmem((2, W, L), f32),
            "send3": vmem((2, 2, PD, L), f32),
            "got3": vmem((2, G, 2, C, L), f32),
            "send4": vmem((2, G, 2, C, L), f32),
            "got4": vmem((2, 2, R, L), f32),
            "ew": vmem((2, 2, 8, L), f32),
            "part": vmem((2, 2, 8, L), f32),
            "red1": vmem((2, G, 2, 8, L), f32),
            "middle": vmem((2, 2, 8, L), f32),
            "red2": vmem((2, self.bands, 2, 8, L), f32),
            "out": vmem((3, self.length, 2 * L), f32),
            "store": dma((3,)),
            "load": dma((10,)),
            "s1": dma((2, 2)),
            "r1": dma((2, 2, 2)),
            "s2": dma((2,)),
            "r2": dma((2, NP)),
            "sm": dma((2,)),
            "rm": dma((2,)),
            "sz": dma((2, 2)),
            "rz": dma((2, 2)),
            "s3": dma((2,)),
            "r3": dma((2, 2, 2)),
            "s4": dma((2, 2)),
            "r4": dma((2, 2)),
            "sw": dma((2,)),
            "rw": dma((2,)),
            "srow": dma,
            "rrow": dma,
            "sedge": dma((2, 2)),
            "redge": dma((2, 2)),
            "szon": dma((2,)),
            "rzon": dma((2,)),
            "sstag": dma,
            "rstag": dma,
            "sa": dma((2,)),
            "ra": dma((2,)),
            "sb": dma((2,)),
            "rb": dma((2,)),
        }


class Refs:
    pass


def kernel(plan, names, *refs):
    (forcing_ref, mask_ref, self_ref, east_ref, north_ref, zonal_ref, aligned_ref, staggered_ref,
     matrix_ref, wave_ref, solution_ref, residual_ref, direction_ref) = refs[:13]
    s = Refs()
    for name, ref in zip(names, refs[13:]):
        setattr(s, name, ref)
    G, NP, C, PD, W, R, L = (
        plan.groups, plan.pairs, plan.chunk, plan.padded, plan.width, plan.rows, plan.block
    )
    bands, length, tile, table = plan.bands, plan.length, plan.tile, plan.table
    half = L // 2
    total = G * length
    f32 = jnp.float32
    band = lax.axis_index("lat")
    me = lax.axis_index("lon")
    pair, core = me // 2, me % 2
    mate = me + 1 - 2 * core
    has_up, has_down = band < bands - 1, band > 0
    sends_up, sends_down = (core == 1) & has_up, (core == 1) & has_down
    STEPS = [(d, e) for d in range(1, NP) for e in (0, 1)] + [(0, 1)]
    CP, sizes = plan.pair_size, plan.sizes
    used = NP * CP
    last_pair, last_at = (length - 1) // CP, (length - 1) % CP
    last_core = 1 if last_at >= sizes[0] else 0
    last_chunk = 2 * last_pair + last_core
    last_at = (last_at - sizes[0] * last_core) // 8 * 8
    pieces = ([[(0, size)] for size in sizes], plan.pieces)
    last_tile = (length - 1) // 8 * 8
    last_row = (length - 1) % 8

    def to_dev(d, e):
        return 2 * ((pair + d) % NP) + (core + e) % 2

    def from_dev(d, e):
        return 2 * ((pair - d + NP) % NP) + (core + e) % 2

    def remote(src, dst, send, recv, device):
        return pltpu.make_async_remote_copy(
            src_ref=src, dst_ref=dst, send_sem=send, recv_sem=recv,
            device_id=device, device_id_type=MESH,
        )

    pending = []

    def launch(make, when=None):
        if when is None:
            make().start()
        else:
            pl.when(when)(lambda: make().start())

    def recv_all(ref, sem, when=None):
        def wait():
            remote(ref, ref, sem, sem, (band, mate)).wait_recv()
        wait() if when is None else pl.when(when)(wait)

    def sent(ref, sem, when=None):
        pending.append((ref, sem, when))

    def drain(keep=0):
        done = len(pending) - keep
        for ref, sem, when in pending[:done]:
            def wait(ref=ref, sem=sem):
                remote(ref, ref, sem, sem, (band, mate)).wait_send()
            wait() if when is None else pl.when(when)(wait)
        del pending[:done]

    def chunks(t, count):
        return s.got3.at[t, pl.ds(0, count)]

    def row_of(index):
        return index // 2 * CP + index % 2 * sizes[0]

    def piece_rows(index, start, count):
        return pl.ds(pl.multiple_of(row_of(index) + start, 8), count)

    def own_of(ref_of, sem, move):
        for c in range(2):
            sent(ref_of(sizes[c]), sem, core == c)
            pl.when(core == c)(functools.partial(move, sizes[c]))

    def for_core(body):
        for c in range(2):
            pl.when(core == c)(functools.partial(body, c))

    def span(index, size=128):
        return pl.ds(pl.multiple_of(index * size, size), size)

    def loop(count, body):
        def step(index, carry):
            body(index)
            return carry
        lax.fori_loop(0, count, step, 0)

    def eight_on(start, count):
        return pl.ds(start + 8 if isinstance(start, int) else pl.multiple_of(start + 8, 8), count)

    def loop_rows(body):
        full = length // 128
        loop(full, lambda index: body(pl.multiple_of(index * 128, 128), 128))
        if length % 128:
            body(full * 128, length % 128)

    def lanes_left(count):
        return lax.broadcasted_iota(jnp.int32, (count, L), 1) < half

    def groups_of(t0, t1):
        mask = lanes_left(t0.shape[0])
        return jnp.where(mask, t1, t0), jnp.where(mask, t0, t1)

    loads = []
    for index, (src, dst) in enumerate((
        (forcing_ref, s.forcing),
        (mask_ref, s.mask),
        (matrix_ref.at[pair], s.matrix),
        (wave_ref.at[pair], s.wave),
        (self_ref, s.selfc),
        (east_ref, s.eastc),
        (north_ref, s.northc),
        (zonal_ref, s.zonal),
        (aligned_ref, s.aligned),
        (staggered_ref, s.staggered),
    )):
        loads.append(pltpu.make_async_copy(src, dst, s.load.at[index]))
    loads[0].start()
    loads[1].start()

    barrier = pltpu.get_barrier_semaphore()
    for d, e in STEPS:
        pl.semaphore_signal(barrier, inc=1, device_id=(band, to_dev(d, e)), device_id_type=MESH)
    for side, has in ((band + 1, has_up), (band - 1, has_down)):
        @pl.when(has)
        def _(side=side):
            pl.semaphore_signal(barrier, inc=1, device_id=(side, me), device_id_type=MESH)

    loads[0].wait()
    loads[1].wait()
    for load in loads[2:]:
        load.start()
    s.xs[0, :, length:R, :] = jnp.zeros((2, R - length, L), f32)
    s.wet[:, 8 + length : 16 + R, :] = jnp.zeros((2, R + 8 - length, L), f32)
    s.field[:, 8 + R : 16 + R, :] = jnp.zeros((2, 8, L), f32)

    def make_rhs(start, count):
        at = pl.ds(start, count)
        wet = s.mask[at, :].astype(f32)
        rhs = wet * s.forcing[at, :]
        a, b = groups_of(rhs[:, :L], rhs[:, L:])
        s.xs[0, 0, at, :] = a
        s.xs[0, 1, at, :] = b
        at8 = eight_on(start, count)
        s.wet[0, at8, :] = wet[:, :L]
        s.wet[1, at8, :] = wet[:, L:]

    loop_rows(make_rhs)
    pl.semaphore_wait(barrier, G - 1 + has_up.astype(jnp.int32) + has_down.astype(jnp.int32))

    def send_phase1(t, g):
        for h in range(len(pieces[t][0])):
            for d in list(range(1, NP)) + [0]:
                for c in range(2):
                    start, count = pieces[t][c][h]

                    def make(d=d, c=c, start=start, count=count):
                        to = 2 * ((pair + d) % NP) + c
                        return remote(s.xs.at[t, g, piece_rows(to, start, count)],
                                      s.got1.at[t, g, me, pl.ds(start, count)],
                                      s.s1.at[t, g], s.r1.at[t, g, h], (band, to))
                    launch(make, None if d else core != c)

        def move(size):
            s.got1[t, g, me, :size, :] = s.xs[t, g, piece_rows(me, 0, size), :]

        own_of(lambda size: s.xs.at[t, g, pl.ds(0, used - size)], s.s1.at[t, g], move)

    def outer_forward(t, g):
        for h in range(len(pieces[t][0])):
            for c in range(2):
                count = pieces[t][c][h][1]
                recv_all(s.got1.at[t, g, pl.ds(0, G - 1), pl.ds(0, count)], s.r1.at[t, g, h],
                         core == c)

            def work(c):
                start, count = pieces[t][c][h]

                def step(index):
                    at = pl.ds(pl.multiple_of(index * 8 + start, 8), 8)
                    values = [s.got1[t, g, place, at, :] for place in range(G)]
                    for row in range(G):
                        s.send2[t, row // 2, g, row % 2, at, :] = weighted(values, table[row])

                loop(count // 8, step)
                for d in list(range(1, NP)) + ([] if c == g else [0]):
                    to = (pair + d) % NP
                    remote(s.send2.at[t, to, g, :, pl.ds(start, count), :],
                           s.cells.at[t, 0, :, piece_rows(me, start, count), :],
                           s.s2.at[t], s.r2.at[t, d], (band, 2 * to + g)).start()

            for_core(work)

        @pl.when(core == g)
        def _():
            s.cells[t, 0, :, piece_rows(me, 0, sizes[g]), :] = s.send2[t, pair, g, :, : sizes[g], :]

    def pair_rows(d):
        return pl.ds(pl.multiple_of((pair - d + NP) % NP * CP, 8), CP)

    def relay(t):
        for d in range(NP):
            if d:
                recv_all(s.send3.at[t, :, pl.ds(0, CP)], s.r2.at[t, d])
            else:
                for c in range(2):
                    recv_all(s.send3.at[t, :, pl.ds(0, sizes[1 - c])], s.r2.at[t, d], core == c)
            at = pair_rows(d)
            @pl.when(core == 1)
            def _():
                low, high = s.cells[t, 0, 0, at, :], s.cells[t, 0, 1, at, :]
                mask = lanes_left(CP)
                s.zs[t, 0, at, :] = jnp.where(mask, low, pltpu.roll(high, half, 1))
                s.zs[t, 1, at, :] = jnp.where(mask, pltpu.roll(low, half, 1), high)

            for way, has in ((0, sends_down), (1, sends_up)):
                def make(way=way):
                    return remote(s.zs.at[t, way, at, :], s.zgot.at[t, way, at, :],
                                  s.sz.at[t, way], s.rz.at[t, way], (band - 1 + 2 * way, me))
                launch(make, has)

    def wait_mate(t):
        recv_all(s.spec_mate.at[t], s.rm.at[t])

    def wait_across(t):
        for way, has in ((0, has_up), (1, has_down)):
            recv_all(s.zgot.at[t, way, pl.ds(0, used)], s.rz.at[t, way], has)

        def step(index):
            size = G // 2 * C
            at = pl.ds(pl.multiple_of(index * size, 8), size)
            above, below = s.zgot[t, 0, at, :], s.zgot[t, 1, at, :]
            mask = lanes_left(size)
            s.cells[t, 1, 0, at, :] = jnp.where(mask, above, pltpu.roll(below, half, 1))
            s.cells[t, 1, 1, at, :] = jnp.where(mask, pltpu.roll(above, half, 1), below)

        loop(2, step)

    def mix_in(t, at, value, which, start):
        gain = s.gain[which * L : (which + 1) * L, :]
        high, low = parted(value)
        wide = dot(high, gain)
        mixed = wide[:, :L] + (wide[:, L:] + dot(low, gain[:, :L]))
        s.mixed[t, at, :] = mixed if start else mixed + s.mixed[t, at, :]

    def transform(t, which):
        hi, lo = parted(s.cells[t, which].reshape(W, L))
        both = jnp.concatenate([hi, lo], axis=1)
        for start in range(0, W, tile):
            at = pl.ds(start, tile)
            wide = dot(s.matrix[0, at, :], both)
            value = wide[:, :L] + (wide[:, L:] + dot(s.matrix[1, at, :], hi))
            value = value * s.scale[which, at, :]
            if which == 0:
                s.spec[t, at, :] = value
                remote(s.spec.at[t, at], s.spec_mate.at[t, at],
                       s.sm.at[t], s.rm.at[t], (band, mate)).start()
            mix_in(t, at, value, which, which == 0)

    def inner_forward(t):
        relay(t)
        for c in range(2):
            sent(s.got3.at[t, pl.ds(0, G - 1), :, pl.ds(0, sizes[c])], s.s2.at[t], core == c)
        sent(s.zgot.at[t, 0, pl.ds(0, used)], s.sz.at[t, 0], sends_down)
        sent(s.zgot.at[t, 1, pl.ds(0, used)], s.sz.at[t, 1], sends_up)
        transform(t, 0)
        sent(s.spec_mate.at[t], s.sm.at[t])

        @pl.when(core == 1)
        def _():
            wait_across(t)
            transform(t, 1)

        wait_mate(t)
        whole = pl.ds(0, W)
        mix_in(t, whole, s.spec_mate[t], 2, False)

    def inner_back(t):
        hi, lo = parted(s.mixed[t] * s.scale_out[...])
        both = jnp.concatenate([hi, lo], axis=1)
        size = NP // 2 * CP
        first = 1 - me // (G // 2)
        for turn in range(2):
            side = first if turn == 0 else 1 - first
            for part in range(2):
                at = pl.ds(pl.multiple_of(part * PD + side * size, 16), size)
                wide = dot(s.turned[0, at, :], both)
                s.send3[t, part, pl.ds(pl.multiple_of(side * size, 8), size), :] = (
                    wide[:, :L] + (wide[:, L:] + dot(s.turned[1, at, :], hi)))
            for h in range(len(plan.pieces[0])):
                for d in list(range(1, NP)) + [0]:
                    for c in range(2):
                        start, count = plan.pieces[c][h]

                        def make(d=d, c=c, start=start, count=count):
                            to = 2 * ((pair + d) % NP) + c
                            return remote(
                                s.send3.at[t, :, piece_rows(to, start, count), :],
                                s.got3.at[t, me, :, pl.ds(start, count), :],
                                s.s3.at[t], s.r3.at[t, core, h], (band, to))
                        here = (2 * ((pair + d) % NP)) // (G // 2) == side
                        launch(make, here if d else here & (core != c))

        def move(size):
            s.got3[t, me, :, :size, :] = s.send3[t, :, piece_rows(me, 0, size), :]

        own_of(lambda size: s.send3.at[t, :, pl.ds(0, used - size)], s.s3.at[t], move)

    def outer_back(t, g, edges):
        for h in range(len(plan.pieces[0])):
            for c in range(2):
                recv_all(s.got3.at[t, pl.ds(0, NP - (c == g)), :, pl.ds(0, plan.pieces[c][h][1]), :],
                         s.r3.at[t, g, h], core == c)

            def work(c):
                start, count = plan.pieces[c][h]

                def step(index):
                    at = pl.ds(pl.multiple_of(index * 8 + start, 8), 8)
                    values = [s.got3[t, 2 * (row // 2) + g, row % 2, at, :] for row in range(G)]
                    for place in range(G):
                        s.send4[t, place, g, at, :] = weighted(values, table[:, place])

                loop(count // 8, step)
                for way, (owner, shift, at) in enumerate(((0, 1, 0), (last_chunk, G - 1, last_at))):
                    if not edges or owner % 2 != c or not start <= at < start + count:
                        continue

                    @pl.when(me == owner)
                    def _(way=way, shift=shift, at=at):
                        for d, e in STEPS:
                            to = to_dev(d, e)
                            remote(s.send4.at[t, (to + shift) % G, g, pl.ds(at, 8), :],
                                   s.ew.at[way, g], s.sw.at[way], s.rw.at[way], (band, to)).start()
                        s.ew[way, g] = s.send4[t, (me + shift) % G, g, pl.ds(at, 8), :]

                for d, e in STEPS:
                    to = to_dev(d, e)
                    remote(s.send4.at[t, to, g, pl.ds(start, count), :],
                           s.got4.at[t, g, piece_rows(me, start, count), :],
                           s.s4.at[t, g], s.r4.at[t, g], (band, to)).start()

            for_core(work)

        def move(size):
            s.got4[t, g, piece_rows(me, 0, size), :] = s.send4[t, me, g, :size, :]

        own_of(lambda size: s.got1.at[t, g, pl.ds(0, G - 1), pl.ds(0, size)], s.s4.at[t, g], move)
        if edges and g == 1:
            for way, owner in enumerate((0, last_chunk)):
                sent(s.red1.at[0, pl.ds(0, G - 1)], s.sw.at[way], me == owner)

    def wait_back(t, g):
        for c in range(2):
            recv_all(s.xs.at[t, g, pl.ds(0, used - sizes[c])], s.r4.at[t, g], core == c)

    def wait_rows():
        for way, owner in enumerate((0, last_chunk)):
            recv_all(s.ew.at[way], s.rw.at[way], me != owner)

    def send_edges(i):
        for way, (side, has) in enumerate(((band - 1, has_down), (band + 1, has_up))):
            def make(way=way, side=side):
                return remote(s.edge_out.at[i, way], s.edge_in.at[i, way],
                              s.sedge.at[i, way], s.redge.at[i, way], (side, me))
            launch(make, has)
            sent(s.edge_out.at[i, way], s.sedge.at[i, way], has)

    def wait_edges(i):
        for way, has in enumerate((has_up, has_down)):
            recv_all(s.edge_in.at[i, way], s.redge.at[i, way], has)

    def column_of(i, way):
        tile8 = s.edge_in[i, way]
        return jnp.concatenate([tile8, jnp.zeros((L - 8, L), f32)], axis=0).T

    def reduce_send(i):
        for d, e in STEPS:
            remote(s.part.at[i], s.red1.at[i, me], s.sa.at[i], s.ra.at[i],
                   (band, to_dev(d, e))).start()
        sent(s.red1.at[i, pl.ds(0, G - 1)], s.sa.at[i])
        s.red1[i, me] = s.part[i]

    def reduce_middle(i):
        recv_all(s.red1.at[i, pl.ds(0, G - 1)], s.ra.at[i])
        value = s.red1[i, 0]
        for place in range(1, G):
            value = value + s.red1[i, place]
        s.middle[i] = value
        s.red2[i, band] = value
        for step in range(1, bands):
            remote(s.middle.at[i], s.red2.at[i, band], s.sb.at[i], s.rb.at[i],
                   ((band + step) % bands, me)).start()
        sent(s.red2.at[i, pl.ds(0, bands - 1)], s.sb.at[i])

    def reduce_end(i):
        recv_all(s.red2.at[i, pl.ds(0, bands - 1)], s.rb.at[i])
        value = s.red2[i, 0]
        for place in range(1, bands):
            value = value + s.red2[i, place]
        return [jnp.sum(value[k], keepdims=True) for k in range(2)]

    def eights(value):
        return value.reshape(value.shape[0] // 8, 8, L).sum(axis=0)

    def weight_of(at):
        wave = s.wave[at, :]
        edge = (wave == 0.0) | (wave == 4.0)
        return jnp.where(edge, np.float32(1.0 / total), np.float32(2.0 / total))

    send_phase1(0, 1)
    send_phase1(0, 0)

    blocks = R // 128

    def shifted(index, by=8):
        return pl.ds(pl.multiple_of(index * 128 + by, 8), 128)

    for load in loads[4:]:
        load.wait()
    for ref in (s.east_wet, s.north):
        ref[:, length:R, :] = jnp.zeros((2, R - length, L), f32)

    def make_faces(start, count):
        at, at8 = pl.ds(start, count), eight_on(start, count)
        for k in range(2):
            lanes = slice(k * L, (k + 1) * L)
            wet = s.wet[k, at8, :]
            s.east_wet[k, at, :] = s.eastc[at, lanes] * wet
            s.north[k, at, :] = s.northc[at, lanes] * wet

    loop_rows(make_faces)
    west_dev, east_dev = (me + G - 1) % G, (me + 1) % G
    s.row_out[0] = s.wet[:, 8:16, :]
    s.row_out[1] = s.wet[:, 8 + last_tile : 16 + last_tile, :]
    s.row_out[2] = s.east_wet[:, last_tile : last_tile + 8, :]
    for k, device in enumerate((west_dev, east_dev, east_dev)):
        remote(s.row_out.at[k], s.row_in.at[k], s.srow, s.rrow, (band, device)).start()
    sent(s.row_in, s.srow)

    def take_edges(i, low, high, by):
        for b in range(blocks):
            s.edge_out[i, 0, b : b + 1, :] = low[pl.ds(128 * b + by[0], 128), :].T[:1, :]
            s.edge_out[i, 1, b : b + 1, :] = high[pl.ds(128 * b + by[1], 128), :].T[L - 1 :, :]
        if blocks < 8:
            s.edge_out[i, :, blocks:, :] = jnp.zeros((2, 8 - blocks, L), f32)

    take_edges(0, s.wet.at[0], s.north.at[1], (8, 0))
    send_edges(0)
    for way, (side, has) in enumerate(((band - 1, has_down), (band + 1, has_up))):
        def send_zonal(way=way, side=side):
            return remote(
                s.zonal, s.zonal_in.at[way], s.szon.at[way], s.rzon.at[way], (side, me))
        launch(send_zonal, has)
        sent(s.zonal, s.szon.at[way], has)

    def send_stag():
        return remote(s.staggered.at[1], s.carried, s.sstag, s.rstag, (band + 1, me))

    launch(send_stag, has_up)
    sent(s.carried, s.sstag, has_up)
    for way, has in enumerate((has_up, has_down)):
        @pl.when(jnp.logical_not(has))
        def _(way=way):
            for i in range(2):
                s.edge_in[i, way] = jnp.zeros((8, L), f32)
                s.zgot[i, way] = jnp.zeros((PD, L), f32)
            s.zonal_in[way] = jnp.zeros((1, 2 * L), f32)

    if PD > used:
        for t in range(2):
            s.cells[t, 0, :, used:, :] = jnp.zeros((2, PD - used, L), f32)
            s.zgot[t, :, used:, :] = jnp.zeros((2, PD - used, L), f32)

    @pl.when(jnp.logical_not(has_down))
    def _():
        s.carried[...] = jnp.zeros((L, L), f32)

    loads[2].wait()
    loads[3].wait()

    def turn(index):
        at = span(index)
        for k in range(2):
            s.turned[k, at, :] = s.matrix[k, :, at].T

    loop(W // 128, turn)

    outer_forward(0, 1)
    outer_forward(0, 0)

    for way, has in enumerate((has_up, has_down)):
        recv_all(s.zonal_in.at[way], s.rzon.at[way], has)
    z0, z1 = s.zonal[:, :L], s.zonal[:, L:]
    mask1 = lanes_left(1)
    zone_a, zone_b = jnp.where(mask1, z1, z0), jnp.where(mask1, z0, z1)
    is_low = core == 0
    zones = (
        jnp.where(is_low, zone_a, zone_b),
        jnp.where(mask1, s.zonal_in[0, :, :L], s.zonal_in[1, :, L:]),
    )

    def make_scale(index):
        at = span(index)
        wave = s.wave[at, :]
        for k, zone in enumerate(zones):
            s.scale[k, at, :] = lax.rsqrt(1.0 + wave * zone)
        s.scale_out[at, :] = s.scale[0, at, :] * weight_of(at)

    loop(W // 128, make_scale)

    recv_all(s.carried, s.rstag, has_down)

    def swapped(value):
        value = jnp.concatenate([value[half:, :], value[:half, :]], axis=0)
        return pltpu.roll(value, half, 1)

    row_top = lax.broadcasted_iota(jnp.int32, (L, L), 0) < half
    col_left = lanes_left(L)
    tl, tr = row_top & col_left, row_top & jnp.logical_not(col_left)
    bl = jnp.logical_not(row_top) & col_left
    br = jnp.logical_not(row_top) & jnp.logical_not(col_left)
    al0, al1 = s.aligned[0], s.aligned[1]
    mid, top, low = swapped(s.staggered[0]), swapped(s.staggered[1]), swapped(s.carried[...])
    zero = jnp.zeros((L, L), f32)

    def pick(*items):
        value = zero
        for where, block in items:
            value = jnp.where(where, block, value)
        return value

    own = jnp.where(
        is_low, mid + pick((tl, al1), (br, al0)), pick((tl, al0 + low), (br, al1 + top)))
    beside = jnp.where(is_low, pick((tr, al0), (bl, al1)), pick((tr, al1), (bl, al0)))
    across = pick((tr, top), (bl, low))
    for k, value in enumerate((own, across, beside)):
        hi, lo = parted(value)
        s.gain[k * L : (k + 1) * L, :L] = hi
        s.gain[k * L : (k + 1) * L, L:] = lo

    inner_forward(0)
    inner_back(0)

    def rz_part(index, carry):
        at = span(index)
        return carry + eights(s.spec[0, at, :] * (s.mixed[0, at, :] * weight_of(at)))

    s.part[0, 0] = lax.fori_loop(0, W // 128, rz_part, jnp.zeros((8, L), f32))

    recv_all(s.row_in, s.rrow)
    wait_edges(0)
    north_col, south_col = column_of(0, 0), column_of(0, 1)
    for k in range(2):
        s.wet[k, 8 + length : 9 + length, :] = s.row_in[0, k, 0:1, :]
        s.east[k, 7:8, :] = s.row_in[2, k, last_row : last_row + 1, :] * s.wet[k, 8:9, :]
    lane = lax.broadcasted_iota(jnp.int32, (128, L), 1)
    first_lane, last_lane = lane == 0, lane == L - 1
    for b in range(blocks):
        at, at8, at9 = pl.ds(128 * b, 128), pl.ds(128 * b + 8, 128), pl.ds(128 * b + 9, 128)
        wet = [s.wet[k, at8, :] for k in range(2)]
        east = [s.east_wet[k, at, :] * s.wet[k, at9, :] for k in range(2)]
        moved = [pltpu.roll(value, L - 1, 1) for value in wet]
        beyond = jnp.broadcast_to(north_col[:, b : b + 1], (128, L))
        north = [
            s.north[0, at, :] * jnp.where(last_lane, moved[1], moved[0]),
            s.north[1, at, :] * jnp.where(last_lane, beyond, moved[1]),
        ]
        moved = [pltpu.roll(value, 1, 1) for value in north]
        beyond = jnp.broadcast_to(south_col[:, b : b + 1], (128, L))
        south = [
            jnp.where(first_lane, beyond * wet[0], moved[0]),
            jnp.where(first_lane, moved[0], moved[1]),
        ]
        for k in range(2):
            s.east[k, at8, :] = east[k]
            s.north[k, at, :] = north[k]
            s.south[k, at, :] = south[k]
    def make_diag(start, count):
        at, at8 = pl.ds(start, count), eight_on(start, count)
        for k in range(2):
            wet = s.wet[k, at8, :]
            own = (1.0 - wet) + wet * s.selfc[at, k * L : (k + 1) * L]
            s.diag[k, at, :] = own + s.diag[k, at, :]

    for b in range(blocks):
        at, at8, at7 = pl.ds(128 * b, 128), pl.ds(128 * b + 8, 128), pl.ds(128 * b + 7, 128)
        for k in range(2):
            s.diag[k, at, :] = (
                (s.east[k, at8, :] + s.east[k, at7, :]) + (s.north[k, at, :] + s.south[k, at, :]))
    s.diag[:, length:R, :] = jnp.zeros((2, R - length, L), f32)
    loop_rows(make_diag)
    for t in range(2):
        for g in range(2):
            if R > used:
                s.got4[t, g, used:, :] = jnp.zeros((R - used, L), f32)

    drain(2)
    outer_back(0, 0, True)
    outer_back(0, 1, True)
    wait_back(0, 0)
    wait_back(0, 1)
    wait_rows()

    def fields_of(t, at, count):
        a, b = s.got4[t, 0, at, :], s.got4[t, 1, at, :]
        mask = lanes_left(count)
        return jnp.where(mask, b, a), jnp.where(mask, a, b)

    def make_field(index):
        at8 = shifted(index)
        for k, value in enumerate(fields_of(0, span(index), 128)):
            s.field[k, at8, :] = s.wet[k, at8, :] * value

    loop(blocks, make_field)
    take_edges(1, s.field.at[0], s.field.at[1], (8, 8))
    send_edges(1)
    mask1 = lanes_left(1)
    for way, (row, source) in enumerate(((0, 0), (last_row, 1))):
        a, b = s.ew[way, 0, row : row + 1, :], s.ew[way, 1, row : row + 1, :]
        for k, value in enumerate((jnp.where(mask1, b, a), jnp.where(mask1, a, b))):
            at = 8 + length if way == 0 else 7
            s.field[k, at : at + 1, :] = s.row_in[source, k, row : row + 1, :] * value

    curvature = jnp.zeros((8, L), f32)
    for b in range(blocks):
        at, at8 = pl.ds(128 * b, 128), pl.ds(128 * b + 8, 128)
        at7, at9 = pl.ds(128 * b + 7, 128), pl.ds(128 * b + 9, 128)
        here = [s.field[k, at8, :] for k in range(2)]
        up = [pltpu.roll(value, L - 1, 1) for value in here]
        down = [pltpu.roll(value, 1, 1) for value in here]
        up = [jnp.where(last_lane, up[1], up[0]), jnp.where(last_lane, 0.0, up[1])]
        down = [jnp.where(first_lane, 0.0, down[0]), jnp.where(first_lane, down[0], down[1])]
        image = []
        for k in range(2):
            value = s.diag[k, at, :] * here[k]
            value = value - s.east[k, at8, :] * s.field[k, at9, :]
            value = value - s.east[k, at7, :] * s.field[k, at7, :]
            value = value - s.north[k, at, :] * up[k]
            value = value - s.south[k, at, :] * down[k]
            if 128 * (b + 1) > length:
                row = lax.broadcasted_iota(jnp.int32, (128, L), 0)
                value = jnp.where(row < length - 128 * b, value, 0.0)
            image.append(value)
            curvature = curvature + eights(here[k] * image[k])
        s.xs[1, 0, at, :], s.xs[1, 1, at, :] = groups_of(*image)

    send_phase1(1, 0)
    drain(2)
    wait_edges(1)
    north_col, south_col = column_of(1, 0), column_of(1, 1)
    for b in range(blocks):
        at, at8 = pl.ds(128 * b, 128), pl.ds(128 * b + 8, 128)
        south = s.south[0, at, :] * jnp.broadcast_to(south_col[:, b : b + 1], (128, L))
        north = s.north[1, at, :] * jnp.broadcast_to(north_col[:, b : b + 1], (128, L))
        extra = jnp.where(first_lane, south, jnp.where(last_lane, north, 0.0))
        s.xs[1, 1, at, :] = s.xs[1, 1, at, :] - extra
        here = jnp.where(first_lane, s.field[0, at8, :], s.field[1, at8, :])
        curvature = curvature - eights(here * extra)
    send_phase1(1, 1)
    s.part[0, 1] = curvature
    reduce_send(0)

    outer_forward(1, 0)
    outer_forward(1, 1)
    reduce_middle(0)
    inner_forward(1)
    inner_back(1)
    rz_now, bend = reduce_end(0)
    alpha = rz_now / bend

    def rz_next_part(index, carry):
        at = span(index)
        spectrum = s.spec[0, at, :] - alpha * s.spec[1, at, :]
        mixed = s.mixed[0, at, :] - alpha * s.mixed[1, at, :]
        return carry + eights(spectrum * (mixed * weight_of(at)))

    s.part[1, 0] = lax.fori_loop(0, W // 128, rz_next_part, jnp.zeros((8, L), f32))
    s.part[1, 1] = jnp.zeros((8, L), f32)
    reduce_send(1)

    drain(3)
    outer_back(1, 0, False)
    outer_back(1, 1, False)
    reduce_middle(1)

    def first_outputs(start, count):
        at, at8 = pl.ds(start, count), eight_on(start, count)
        mask = lanes_left(count)
        rest = [s.xs[0, g, at, :] - alpha * s.xs[1, g, at, :] for g in range(2)]
        s.out[1, at, :L] = jnp.where(mask, rest[1], rest[0])
        s.out[1, at, L:] = jnp.where(mask, rest[0], rest[1])
        for k in range(2):
            s.out[0, at, k * L : (k + 1) * L] = alpha * s.field[k, at8, :]

    loop_rows(first_outputs)
    stores = [
        pltpu.make_async_copy(s.out.at[k], ref, s.store.at[k])
        for k, ref in enumerate((solution_ref, residual_ref, direction_ref))
    ]
    stores[0].start()
    stores[1].start()
    rz_next, _ = reduce_end(1)
    beta = rz_next / rz_now
    wait_back(1, 0)
    drain()
    wait_back(1, 1)

    def last_output(start, count):
        at, at8 = pl.ds(start, count), eight_on(start, count)
        for k, value in enumerate(fields_of(1, at, count)):
            first = s.field[k, at8, :]
            second = first - alpha * (s.wet[k, at8, :] * value)
            s.out[2, at, k * L : (k + 1) * L] = second + beta * first

    loop_rows(last_output)
    stores[2].start()
    for store in stores:
        store.wait()
    drain()


def finish_kernel(*refs):
    ins, outs, held, arrived, left = refs[:3], refs[3:6], refs[6], refs[7], refs[8]
    gets = [pltpu.make_async_copy(ref, held.at[k], arrived.at[k]) for k, ref in enumerate(ins)]
    puts = [pltpu.make_async_copy(held.at[k], ref, left.at[k]) for k, ref in enumerate(outs)]
    for get in gets:
        get.start()
    for get, put in zip(gets, puts):
        get.wait()
        put.start()
    for put in puts:
        put.wait()


def local(
    surface_forcing,
    ocean_mask,
    self_coupling,
    east_coupling,
    north_coupling,
    zonal_weight,
    aligned_inverse,
    staggered_inverse,
):
    groups, bands = lax.axis_size("lon"), lax.axis_size("lat")
    length, columns = surface_forcing.shape
    block = aligned_inverse.shape[1]
    assert columns == 2 * block and block == 128 and groups % 4 == 0
    chunk = -(-length // (8 * groups)) * 8
    padded = groups * chunk
    while 2 * padded % 128:
        chunk, padded = chunk + 8, padded + 8 * groups
    plan = Plan(groups, bands, length, columns, block, (chunk, padded))
    assert plan.rows <= 1024
    matrix, waves = inner_tables(groups, length, padded)
    lanes = np.repeat(waves[:, :, None], block, axis=2)
    scratch = plan.scratch()
    anywhere = pl.BlockSpec(memory_space=pl.ANY)
    shape = jax.ShapeDtypeStruct((length, columns), jnp.float32)
    outs = pl.pallas_call(
        functools.partial(kernel, plan, tuple(scratch)),
        out_shape=(shape,) * 3,
        in_specs=[anywhere] * 10,
        out_specs=(anywhere,) * 3,
        scratch_shapes=list(scratch.values()),
        compiler_params=pltpu.CompilerParams(
            collective_id=0, has_side_effects=True, vmem_limit_bytes=61 * 2**20
        ),
        name="step",
    )(
        surface_forcing, ocean_mask, self_coupling, east_coupling, north_coupling,
        zonal_weight[None, :], aligned_inverse, staggered_inverse,
        jnp.asarray(matrix), jnp.asarray(lanes),
    )
    return pl.pallas_call(
        finish_kernel,
        out_shape=(shape,) * 3,
        in_specs=[anywhere] * 3,
        out_specs=(anywhere,) * 3,
        scratch_shapes=[
            pltpu.VMEM((3, length, columns), jnp.float32),
            pltpu.SemaphoreType.DMA((3,)),
            pltpu.SemaphoreType.DMA((3,)),
        ],
        name="finish",
    )(*outs)


def solution(mesh):
    grid = P("lon", "lat")
    stack = P("lat", None, None)
    return jax.shard_map(
        local,
        mesh=mesh,
        in_specs=(grid, grid, grid, grid, grid, P("lat"), stack, stack),
        out_specs=(grid, grid, grid),
        check_vma=False,
    )
```

```python
import functools

import jax
import jax.numpy as jnp
import numpy as np
from jax import lax
from jax.experimental import pallas as pl
from jax.experimental.pallas import tpu as pltpu
from jax.sharding import PartitionSpec as P

MESH = pl.DeviceIdType.MESH
TILE = 576


def outer_table(groups):
    table = np.zeros((groups, groups))
    place = np.arange(groups)
    table[0] = 1.0
    table[1] = np.where(place % 2 == 0, 1.0, -1.0)
    for mode in range(1, groups // 2):
        turn = 2.0 * np.pi * (mode * place % groups) / groups
        table[2 * mode] = np.cos(turn)
        table[2 * mode + 1] = -np.sin(turn)
    table[np.abs(table) < 1e-12] = 0.0
    return table


def inner_tables(groups, length, padded):
    total = groups * length
    pairs = groups // 2
    matrix = np.zeros((pairs, 2 * padded, 2 * padded))
    waves = np.zeros((pairs, 2 * padded))
    cell = np.arange(length)

    def turns(modes):
        return 2.0 * np.pi * (modes[:, None] * cell[None, :] % total) / total

    def note(pair, start, modes):
        stop = start + len(modes)
        waves[pair, start:stop] = 2.0 - 2.0 * np.cos(2.0 * np.pi * modes / total)

    for part, (first, real_count) in enumerate(((0, length // 2 + 1), (groups // 2, (length + 1) // 2))):
        skipped = 1 if part == 0 else 0
        real = first + groups * np.arange(real_count)
        imag = first + groups * (skipped + np.arange(length - real_count))
        row = part * padded
        columns = slice(part * padded, part * padded + length)
        matrix[0, row : row + real_count, columns] = np.cos(turns(real))
        matrix[0, row + real_count : row + length, columns] = -np.sin(turns(imag))
        note(0, row, real)
        note(0, row + real_count, imag)
    for pair in range(1, pairs):
        modes = pair + groups * np.arange(length)
        angle = turns(modes)
        low, high = slice(0, length), slice(padded, padded + length)
        matrix[pair, low, low] = np.cos(angle)
        matrix[pair, low, high] = np.sin(angle)
        matrix[pair, high, low] = -np.sin(angle)
        matrix[pair, high, high] = np.cos(angle)
        note(pair, 0, modes)
        note(pair, padded, modes)
    single = matrix.astype(np.float32)
    leading = single.astype(jnp.bfloat16)
    rest = (matrix - leading.astype(np.float64)).astype(jnp.bfloat16)
    return np.stack([leading, rest], axis=1), waves.astype(np.float32)


def parted(value):
    leading = value.astype(jnp.bfloat16)
    return leading, (value - leading.astype(jnp.float32)).astype(jnp.bfloat16)


def dot(left, right):
    return jnp.dot(left, right, preferred_element_type=jnp.float32)


def weighted(values, factors):
    total = None
    for value, factor in zip(values, factors):
        if factor == 0.0:
            continue
        term = value if factor == 1.0 else value * np.float32(factor)
        total = term if total is None else total + term
    return total


class Plan:
    def __init__(self, groups, bands, length, columns, block, width_of):
        self.groups, self.bands, self.length = groups, bands, length
        self.pairs = groups // 2
        self.columns, self.block = columns, block
        self.chunk, self.padded = width_of
        self.width = 2 * self.padded
        self.rows = max(-(-length // 128) * 128, -(-self.padded // 128) * 128)
        self.tile = next(t for t in (TILE, 384, 256, 128) if self.width % t == 0)
        self.table = outer_table(groups)
        tiles = -(-(-(-length // 8)) // self.pairs)
        self.pair_size = 8 * tiles
        self.sizes = (-(-tiles // 2) * 8, tiles // 2 * 8)
        assert self.sizes[0] <= self.chunk and self.sizes[1] > 0
        self.pieces = []
        for size in self.sizes:
            cut = -(-size // 16) * 8
            self.pieces.append([(0, cut)] + ([(cut, size - cut)] if cut < size else []))

    def scratch(self):
        f32, bf16 = jnp.float32, jnp.bfloat16
        G, NP, C, PD, W, R, L = (
            self.groups, self.pairs, self.chunk, self.padded, self.width, self.rows, self.block
        )
        vmem, dma = pltpu.VMEM, pltpu.SemaphoreType.DMA
        return {
            "forcing": vmem((self.length, 2 * L), f32),
            "mask": vmem((self.length, 2 * L), jnp.int32),
            "selfc": vmem((self.length, 2 * L), f32),
            "eastc": vmem((self.length, 2 * L), f32),
            "northc": vmem((self.length, 2 * L), f32),
            "zonal": vmem((1, 2 * L), f32),
            "zonal_in": vmem((2, 1, 2 * L), f32),
            "aligned": vmem((2, L, L), f32),
            "staggered": vmem((2, L, L), f32),
            "carried": vmem((L, L), f32),
            "matrix": vmem((2, W, W), bf16),
            "turned": vmem((2, W, W), bf16),
            "wave": vmem((W, L), f32),
            "wet": vmem((2, R + 16, L), f32),
            "east_wet": vmem((2, R, L), f32),
            "east": vmem((2, R + 16, L), f32),
            "north": vmem((2, R, L), f32),
            "south": vmem((2, R, L), f32),
            "diag": vmem((2, R, L), f32),
            "field": vmem((2, R + 16, L), f32),
            "row_in": vmem((3, 2, 8, L), f32),
            "row_out": vmem((3, 2, 8, L), f32),
            "edge_out": vmem((2, 2, 8, L), f32),
            "edge_in": vmem((2, 2, 8, L), f32),
            "scale": vmem((2, W, L), f32),
            "scale_out": vmem((W, L), f32),
            "gain": vmem((3 * L, 2 * L), bf16),
            "xs": vmem((2, 2, R, L), f32),
            "got1": vmem((2, 2, G, C, L), f32),
            "send2": vmem((2, NP, 2, 2, C, L), f32),
            "cells": vmem((2, 2, 2, PD, L), f32),
            "zs": vmem((2, 2, PD, L), f32),
            "zgot": vmem((2, 2, PD, L), f32),
            "spec": vmem((2, W, L), f32),
            "spec_mate": vmem((2, W, L), f32),
            "mixed": vmem((2, W, L), f32),
            "send3": vmem((2, 2, PD, L), f32),
            "got3": vmem((2, G, 2, C, L), f32),
            "send4": vmem((2, G, 2, C, L), f32),
            "got4": vmem((2, 2, R, L), f32),
            "ew": vmem((2, 2, 8, L), f32),
            "part": vmem((2, 2, 8, L), f32),
            "red1": vmem((2, G, 2, 8, L), f32),
            "middle": vmem((2, 2, 8, L), f32),
            "red2": vmem((2, self.bands, 2, 8, L), f32),
            "out": vmem((3, self.length, 2 * L), f32),
            "store": dma((3,)),
            "load": dma((10,)),
            "s1": dma((2, 2)),
            "r1": dma((2, 2, 2)),
            "s2": dma((2,)),
            "r2": dma((2, NP)),
            "sm": dma((2,)),
            "rm": dma((2,)),
            "sz": dma((2, 2)),
            "rz": dma((2, 2)),
            "s3": dma((2,)),
            "r3": dma((2, 2, 2)),
            "s4": dma((2, 2)),
            "r4": dma((2, 2)),
            "sw": dma((2,)),
            "rw": dma((2,)),
            "srow": dma,
            "rrow": dma,
            "sedge": dma((2, 2)),
            "redge": dma((2, 2)),
            "szon": dma((2,)),
            "rzon": dma((2,)),
            "sstag": dma,
            "rstag": dma,
            "sa": dma((2,)),
            "ra": dma((2,)),
            "sb": dma((2,)),
            "rb": dma((2,)),
        }


class Refs:
    pass


def kernel(plan, names, *refs):
    (forcing_ref, mask_ref, self_ref, east_ref, north_ref, zonal_ref, aligned_ref, staggered_ref,
     matrix_ref, wave_ref, solution_ref, residual_ref, direction_ref) = refs[:13]
    s = Refs()
    for name, ref in zip(names, refs[13:]):
        setattr(s, name, ref)
    G, NP, C, PD, W, R, L = (
        plan.groups, plan.pairs, plan.chunk, plan.padded, plan.width, plan.rows, plan.block
    )
    bands, length, tile, table = plan.bands, plan.length, plan.tile, plan.table
    half = L // 2
    total = G * length
    f32 = jnp.float32
    band = lax.axis_index("lat")
    me = lax.axis_index("lon")
    pair, core = me // 2, me % 2
    mate = me + 1 - 2 * core
    has_up, has_down = band < bands - 1, band > 0
    sends_up, sends_down = (core == 1) & has_up, (core == 1) & has_down
    if NP == 4:
        across_both = (2 * NP - 1 - 2 * pair) % NP
        OTHERS = [across_both, NP - across_both, 2]
    else:
        OTHERS = list(range(1, NP))
    STEPS = [(d, e) for d in OTHERS for e in (0, 1)] + [(0, 1)]
    CP, sizes = plan.pair_size, plan.sizes
    used = NP * CP
    last_pair, last_at = (length - 1) // CP, (length - 1) % CP
    last_core = 1 if last_at >= sizes[0] else 0
    last_chunk = 2 * last_pair + last_core
    last_at = (last_at - sizes[0] * last_core) // 8 * 8
    pieces = ([[(0, size)] for size in sizes], plan.pieces)
    last_tile = (length - 1) // 8 * 8
    last_row = (length - 1) % 8

    def to_dev(d, e):
        return 2 * ((pair + d) % NP) + (core + e) % 2

    def from_dev(d, e):
        return 2 * ((pair - d + NP) % NP) + (core + e) % 2

    def remote(src, dst, send, recv, device):
        return pltpu.make_async_remote_copy(
            src_ref=src, dst_ref=dst, send_sem=send, recv_sem=recv,
            device_id=device, device_id_type=MESH,
        )

    pending = []

    def launch(make, when=None):
        if when is None:
            make().start()
        else:
            pl.when(when)(lambda: make().start())

    def recv_all(ref, sem, when=None):
        def wait():
            remote(ref, ref, sem, sem, (band, mate)).wait_recv()
        wait() if when is None else pl.when(when)(wait)

    def sent(ref, sem, when=None):
        pending.append((ref, sem, when))

    def drain(keep=0):
        done = len(pending) - keep
        for ref, sem, when in pending[:done]:
            def wait(ref=ref, sem=sem):
                remote(ref, ref, sem, sem, (band, mate)).wait_send()
            wait() if when is None else pl.when(when)(wait)
        del pending[:done]

    def chunks(t, count):
        return s.got3.at[t, pl.ds(0, count)]

    def row_of(index):
        return index // 2 * CP + index % 2 * sizes[0]

    def piece_rows(index, start, count):
        return pl.ds(pl.multiple_of(row_of(index) + start, 8), count)

    def own_of(ref_of, sem, move):
        for c in range(2):
            sent(ref_of(sizes[c]), sem, core == c)
            pl.when(core == c)(functools.partial(move, sizes[c]))

    def for_core(body):
        for c in range(2):
            pl.when(core == c)(functools.partial(body, c))

    def span(index, size=128):
        return pl.ds(pl.multiple_of(index * size, size), size)

    def loop(count, body):
        def step(index, carry):
            body(index)
            return carry
        lax.fori_loop(0, count, step, 0)

    def eight_on(start, count):
        return pl.ds(start + 8 if isinstance(start, int) else pl.multiple_of(start + 8, 8), count)

    def loop_rows(body):
        full = length // 128
        loop(full, lambda index: body(pl.multiple_of(index * 128, 128), 128))
        if length % 128:
            body(full * 128, length % 128)

    def lanes_left(count):
        return lax.broadcasted_iota(jnp.int32, (count, L), 1) < half

    def groups_of(t0, t1):
        mask = lanes_left(t0.shape[0])
        return jnp.where(mask, t1, t0), jnp.where(mask, t0, t1)

    loads = []
    for index, (src, dst) in enumerate((
        (forcing_ref, s.forcing),
        (mask_ref, s.mask),
        (matrix_ref.at[pair], s.matrix),
        (wave_ref.at[pair], s.wave),
        (self_ref, s.selfc),
        (east_ref, s.eastc),
        (north_ref, s.northc),
        (zonal_ref, s.zonal),
        (aligned_ref, s.aligned),
        (staggered_ref, s.staggered),
    )):
        loads.append(pltpu.make_async_copy(src, dst, s.load.at[index]))
    loads[0].start()
    loads[1].start()

    barrier = pltpu.get_barrier_semaphore()
    for d, e in STEPS:
        pl.semaphore_signal(barrier, inc=1, device_id=(band, to_dev(d, e)), device_id_type=MESH)
    for side, has in ((band + 1, has_up), (band - 1, has_down)):
        @pl.when(has)
        def _(side=side):
            pl.semaphore_signal(barrier, inc=1, device_id=(side, me), device_id_type=MESH)

    loads[0].wait()
    loads[1].wait()
    for load in loads[2:]:
        load.start()
    s.xs[0, :, length:R, :] = jnp.zeros((2, R - length, L), f32)
    s.wet[:, 8 + length : 16 + R, :] = jnp.zeros((2, R + 8 - length, L), f32)
    s.field[:, 8 + R : 16 + R, :] = jnp.zeros((2, 8, L), f32)

    def make_rhs(start, count):
        at = pl.ds(start, count)
        wet = s.mask[at, :].astype(f32)
        rhs = wet * s.forcing[at, :]
        a, b = groups_of(rhs[:, :L], rhs[:, L:])
        s.xs[0, 0, at, :] = a
        s.xs[0, 1, at, :] = b
        at8 = eight_on(start, count)
        s.wet[0, at8, :] = wet[:, :L]
        s.wet[1, at8, :] = wet[:, L:]

    loop_rows(make_rhs)
    pl.semaphore_wait(barrier, G - 1 + has_up.astype(jnp.int32) + has_down.astype(jnp.int32))

    def send_phase1(t, g):
        for h in range(len(pieces[t][0])):
            for d in OTHERS + [None]:
                for c in range(2):
                    start, count = pieces[t][c][h]

                    def make(d=d, c=c, start=start, count=count):
                        to = 2 * (pair if d is None else (pair + d) % NP) + c
                        return remote(s.xs.at[t, g, piece_rows(to, start, count)],
                                      s.got1.at[t, g, me, pl.ds(start, count)],
                                      s.s1.at[t, g], s.r1.at[t, g, h], (band, to))
                    launch(make, core != c if d is None else None)

        def move(size):
            s.got1[t, g, me, :size, :] = s.xs[t, g, piece_rows(me, 0, size), :]

        own_of(lambda size: s.xs.at[t, g, pl.ds(0, used - size)], s.s1.at[t, g], move)

    def outer_forward(t, g):
        for h in range(len(pieces[t][0])):
            for c in range(2):
                count = pieces[t][c][h][1]
                recv_all(s.got1.at[t, g, pl.ds(0, G - 1), pl.ds(0, count)], s.r1.at[t, g, h],
                         core == c)

            def work(c):
                start, count = pieces[t][c][h]

                def step(index):
                    at = pl.ds(pl.multiple_of(index * 8 + start, 8), 8)
                    values = [s.got1[t, g, place, at, :] for place in range(G)]
                    for row in range(G):
                        s.send2[t, row // 2, g, row % 2, at, :] = weighted(values, table[row])

                loop(count // 8, step)
                for d in OTHERS + ([] if c == g else [0]):
                    to = (pair + d) % NP
                    remote(s.send2.at[t, to, g, :, pl.ds(start, count), :],
                           s.cells.at[t, 0, :, piece_rows(me, start, count), :],
                           s.s2.at[t], s.r2.at[t, d], (band, 2 * to + g)).start()

            for_core(work)

        @pl.when(core == g)
        def _():
            s.cells[t, 0, :, piece_rows(me, 0, sizes[g]), :] = s.send2[t, pair, g, :, : sizes[g], :]

    def pair_rows(d):
        return pl.ds(pl.multiple_of((pair - d + NP) % NP * CP, 8), CP)

    def relay(t):
        for d in range(NP):
            if d:
                recv_all(s.send3.at[t, :, pl.ds(0, CP)], s.r2.at[t, d])
            else:
                for c in range(2):
                    recv_all(s.send3.at[t, :, pl.ds(0, sizes[1 - c])], s.r2.at[t, d], core == c)
            at = pair_rows(d)
            @pl.when(core == 1)
            def _():
                low, high = s.cells[t, 0, 0, at, :], s.cells[t, 0, 1, at, :]
                mask = lanes_left(CP)
                s.zs[t, 0, at, :] = jnp.where(mask, low, pltpu.roll(high, half, 1))
                s.zs[t, 1, at, :] = jnp.where(mask, pltpu.roll(low, half, 1), high)

            for way, has in ((0, sends_down), (1, sends_up)):
                def make(way=way):
                    return remote(s.zs.at[t, way, at, :], s.zgot.at[t, way, at, :],
                                  s.sz.at[t, way], s.rz.at[t, way], (band - 1 + 2 * way, me))
                launch(make, has)

    def wait_mate(t):
        recv_all(s.spec_mate.at[t], s.rm.at[t])

    def wait_across(t):
        for way, has in ((0, has_up), (1, has_down)):
            recv_all(s.zgot.at[t, way, pl.ds(0, used)], s.rz.at[t, way], has)

        def step(index):
            size = G // 2 * C
            at = pl.ds(pl.multiple_of(index * size, 8), size)
            above, below = s.zgot[t, 0, at, :], s.zgot[t, 1, at, :]
            mask = lanes_left(size)
            s.cells[t, 1, 0, at, :] = jnp.where(mask, above, pltpu.roll(below, half, 1))
            s.cells[t, 1, 1, at, :] = jnp.where(mask, pltpu.roll(above, half, 1), below)

        loop(2, step)

    def mix_in(t, at, value, which, start):
        gain = s.gain[which * L : (which + 1) * L, :]
        high, low = parted(value)
        wide = dot(high, gain)
        mixed = wide[:, :L] + (wide[:, L:] + dot(low, gain[:, :L]))
        s.mixed[t, at, :] = mixed if start else mixed + s.mixed[t, at, :]

    def transform(t, which):
        hi, lo = parted(s.cells[t, which].reshape(W, L))
        both = jnp.concatenate([hi, lo], axis=1)
        for start in range(0, W, tile):
            at = pl.ds(start, tile)
            wide = dot(s.matrix[0, at, :], both)
            value = wide[:, :L] + (wide[:, L:] + dot(s.matrix[1, at, :], hi))
            value = value * s.scale[which, at, :]
            if which == 0:
                s.spec[t, at, :] = value
                remote(s.spec.at[t, at], s.spec_mate.at[t, at],
                       s.sm.at[t], s.rm.at[t], (band, mate)).start()
            mix_in(t, at, value, which, which == 0)

    def inner_forward(t):
        relay(t)
        for c in range(2):
            sent(s.got3.at[t, pl.ds(0, G - 1), :, pl.ds(0, sizes[c])], s.s2.at[t], core == c)
        sent(s.zgot.at[t, 0, pl.ds(0, used)], s.sz.at[t, 0], sends_down)
        sent(s.zgot.at[t, 1, pl.ds(0, used)], s.sz.at[t, 1], sends_up)
        transform(t, 0)
        sent(s.spec_mate.at[t], s.sm.at[t])

        @pl.when(core == 1)
        def _():
            wait_across(t)
            transform(t, 1)

        wait_mate(t)
        whole = pl.ds(0, W)
        mix_in(t, whole, s.spec_mate[t], 2, False)

    def inner_back(t, between=None):
        hi, lo = parted(s.mixed[t] * s.scale_out[...])
        both = jnp.concatenate([hi, lo], axis=1)
        size = NP // 2 * CP
        first = 1 - me // (G // 2)
        for turn in range(2):
            side = first if turn == 0 else 1 - first
            for part in range(2):
                at = pl.ds(pl.multiple_of(part * PD + side * size, 16), size)
                wide = dot(s.turned[0, at, :], both)
                s.send3[t, part, pl.ds(pl.multiple_of(side * size, 8), size), :] = (
                    wide[:, :L] + (wide[:, L:] + dot(s.turned[1, at, :], hi)))
            for h in range(len(plan.pieces[0])):
                for d in OTHERS + [None]:
                    for c in range(2):
                        start, count = plan.pieces[c][h]

                        def make(d=d, c=c, start=start, count=count):
                            to = 2 * (pair if d is None else (pair + d) % NP) + c
                            return remote(
                                s.send3.at[t, :, piece_rows(to, start, count), :],
                                s.got3.at[t, me, :, pl.ds(start, count), :],
                                s.s3.at[t], s.r3.at[t, core, h], (band, to))
                        target = pair if d is None else (pair + d) % NP
                        here = target // (NP // 2) == side
                        launch(make, here & (core != c) if d is None else here)
            if between is not None and turn == 0:
                between()

        def move(size):
            s.got3[t, me, :, :size, :] = s.send3[t, :, piece_rows(me, 0, size), :]

        own_of(lambda size: s.send3.at[t, :, pl.ds(0, used - size)], s.s3.at[t], move)

    def outer_back(t, g, edges):
        for h in range(len(plan.pieces[0])):
            for c in range(2):
                recv_all(s.got3.at[t, pl.ds(0, NP - (c == g)), :, pl.ds(0, plan.pieces[c][h][1]), :],
                         s.r3.at[t, g, h], core == c)

            def work(c):
                start, count = plan.pieces[c][h]

                def step(index):
                    at = pl.ds(pl.multiple_of(index * 8 + start, 8), 8)
                    values = [s.got3[t, 2 * (row // 2) + g, row % 2, at, :] for row in range(G)]
                    for place in range(G):
                        s.send4[t, place, g, at, :] = weighted(values, table[:, place])

                loop(count // 8, step)
                for way, (owner, shift, at) in enumerate(((0, 1, 0), (last_chunk, G - 1, last_at))):
                    if not edges or owner % 2 != c or not start <= at < start + count:
                        continue

                    @pl.when(me == owner)
                    def _(way=way, shift=shift, at=at):
                        for d, e in STEPS:
                            to = to_dev(d, e)
                            remote(s.send4.at[t, (to + shift) % G, g, pl.ds(at, 8), :],
                                   s.ew.at[way, g], s.sw.at[way], s.rw.at[way], (band, to)).start()
                        s.ew[way, g] = s.send4[t, (me + shift) % G, g, pl.ds(at, 8), :]

                for d, e in STEPS:
                    to = to_dev(d, e)
                    remote(s.send4.at[t, to, g, pl.ds(start, count), :],
                           s.got4.at[t, g, piece_rows(me, start, count), :],
                           s.s4.at[t, g], s.r4.at[t, g], (band, to)).start()

            for_core(work)

        def move(size):
            s.got4[t, g, piece_rows(me, 0, size), :] = s.send4[t, me, g, :size, :]

        own_of(lambda size: s.got1.at[t, g, pl.ds(0, G - 1), pl.ds(0, size)], s.s4.at[t, g], move)
        if edges and g == 1:
            for way, owner in enumerate((0, last_chunk)):
                sent(s.red1.at[0, pl.ds(0, G - 1)], s.sw.at[way], me == owner)

    def wait_back(t, g):
        for c in range(2):
            recv_all(s.xs.at[t, g, pl.ds(0, used - sizes[c])], s.r4.at[t, g], core == c)

    def wait_rows():
        for way, owner in enumerate((0, last_chunk)):
            recv_all(s.ew.at[way], s.rw.at[way], me != owner)

    def send_edges(i):
        for way, (side, has) in enumerate(((band - 1, has_down), (band + 1, has_up))):
            def make(way=way, side=side):
                return remote(s.edge_out.at[i, way], s.edge_in.at[i, way],
                              s.sedge.at[i, way], s.redge.at[i, way], (side, me))
            launch(make, has)
            sent(s.edge_out.at[i, way], s.sedge.at[i, way], has)

    def wait_edges(i):
        for way, has in enumerate((has_up, has_down)):
            recv_all(s.edge_in.at[i, way], s.redge.at[i, way], has)

    def column_of(i, way):
        tile8 = s.edge_in[i, way]
        return jnp.concatenate([tile8, jnp.zeros((L - 8, L), f32)], axis=0).T

    def reduce_send(i):
        for d, e in STEPS:
            remote(s.part.at[i], s.red1.at[i, me], s.sa.at[i], s.ra.at[i],
                   (band, to_dev(d, e))).start()
        sent(s.red1.at[i, pl.ds(0, G - 1)], s.sa.at[i])
        s.red1[i, me] = s.part[i]

    def reduce_middle(i):
        recv_all(s.red1.at[i, pl.ds(0, G - 1)], s.ra.at[i])
        value = s.red1[i, 0]
        for place in range(1, G):
            value = value + s.red1[i, place]
        s.middle[i] = value
        s.red2[i, band] = value
        for step in range(1, bands):
            remote(s.middle.at[i], s.red2.at[i, band], s.sb.at[i], s.rb.at[i],
                   ((band + step) % bands, me)).start()
        sent(s.red2.at[i, pl.ds(0, bands - 1)], s.sb.at[i])

    def reduce_end(i):
        recv_all(s.red2.at[i, pl.ds(0, bands - 1)], s.rb.at[i])
        value = s.red2[i, 0]
        for place in range(1, bands):
            value = value + s.red2[i, place]
        return [jnp.sum(value[k], keepdims=True) for k in range(2)]

    def eights(value):
        return value.reshape(value.shape[0] // 8, 8, L).sum(axis=0)

    def weight_of(at):
        wave = s.wave[at, :]
        edge = (wave == 0.0) | (wave == 4.0)
        return jnp.where(edge, np.float32(1.0 / total), np.float32(2.0 / total))

    send_phase1(0, 1)
    send_phase1(0, 0)

    blocks = R // 128

    def shifted(index, by=8):
        return pl.ds(pl.multiple_of(index * 128 + by, 8), 128)

    for load in loads[4:]:
        load.wait()
    for ref in (s.east_wet, s.north):
        ref[:, length:R, :] = jnp.zeros((2, R - length, L), f32)

    def make_faces(start, count):
        at, at8 = pl.ds(start, count), eight_on(start, count)
        for k in range(2):
            lanes = slice(k * L, (k + 1) * L)
            wet = s.wet[k, at8, :]
            s.east_wet[k, at, :] = s.eastc[at, lanes] * wet
            s.north[k, at, :] = s.northc[at, lanes] * wet

    loop_rows(make_faces)
    west_dev, east_dev = (me + G - 1) % G, (me + 1) % G
    s.row_out[0] = s.wet[:, 8:16, :]
    s.row_out[1] = s.wet[:, 8 + last_tile : 16 + last_tile, :]
    s.row_out[2] = s.east_wet[:, last_tile : last_tile + 8, :]
    for k, device in enumerate((west_dev, east_dev, east_dev)):
        remote(s.row_out.at[k], s.row_in.at[k], s.srow, s.rrow, (band, device)).start()
    sent(s.row_in, s.srow)

    def take_edges(i, low, high, by):
        for b in range(blocks):
            s.edge_out[i, 0, b : b + 1, :] = low[pl.ds(128 * b + by[0], 128), :].T[:1, :]
            s.edge_out[i, 1, b : b + 1, :] = high[pl.ds(128 * b + by[1], 128), :].T[L - 1 :, :]
        if blocks < 8:
            s.edge_out[i, :, blocks:, :] = jnp.zeros((2, 8 - blocks, L), f32)

    take_edges(0, s.wet.at[0], s.north.at[1], (8, 0))
    send_edges(0)
    for way, (side, has) in enumerate(((band - 1, has_down), (band + 1, has_up))):
        def send_zonal(way=way, side=side):
            return remote(
                s.zonal, s.zonal_in.at[way], s.szon.at[way], s.rzon.at[way], (side, me))
        launch(send_zonal, has)
        sent(s.zonal, s.szon.at[way], has)

    def send_stag():
        return remote(s.staggered.at[1], s.carried, s.sstag, s.rstag, (band + 1, me))

    launch(send_stag, has_up)
    sent(s.carried, s.sstag, has_up)
    for way, has in enumerate((has_up, has_down)):
        @pl.when(jnp.logical_not(has))
        def _(way=way):
            for i in range(2):
                s.edge_in[i, way] = jnp.zeros((8, L), f32)
                s.zgot[i, way] = jnp.zeros((PD, L), f32)
            s.zonal_in[way] = jnp.zeros((1, 2 * L), f32)

    if PD > used:
        for t in range(2):
            s.cells[t, 0, :, used:, :] = jnp.zeros((2, PD - used, L), f32)
            s.zgot[t, :, used:, :] = jnp.zeros((2, PD - used, L), f32)

    @pl.when(jnp.logical_not(has_down))
    def _():
        s.carried[...] = jnp.zeros((L, L), f32)

    loads[2].wait()
    loads[3].wait()

    def turn(index):
        at = span(index)
        for k in range(2):
            s.turned[k, at, :] = s.matrix[k, :, at].T

    loop(W // 128, turn)

    outer_forward(0, 1)
    outer_forward(0, 0)

    for way, has in enumerate((has_up, has_down)):
        recv_all(s.zonal_in.at[way], s.rzon.at[way], has)
    z0, z1 = s.zonal[:, :L], s.zonal[:, L:]
    mask1 = lanes_left(1)
    zone_a, zone_b = jnp.where(mask1, z1, z0), jnp.where(mask1, z0, z1)
    is_low = core == 0
    zones = (
        jnp.where(is_low, zone_a, zone_b),
        jnp.where(mask1, s.zonal_in[0, :, :L], s.zonal_in[1, :, L:]),
    )

    def make_scale(index):
        at = span(index)
        wave = s.wave[at, :]
        for k, zone in enumerate(zones):
            s.scale[k, at, :] = lax.rsqrt(1.0 + wave * zone)
        s.scale_out[at, :] = s.scale[0, at, :] * weight_of(at)

    loop(W // 128, make_scale)

    recv_all(s.carried, s.rstag, has_down)

    def swapped(value):
        value = jnp.concatenate([value[half:, :], value[:half, :]], axis=0)
        return pltpu.roll(value, half, 1)

    row_top = lax.broadcasted_iota(jnp.int32, (L, L), 0) < half
    col_left = lanes_left(L)
    tl, tr = row_top & col_left, row_top & jnp.logical_not(col_left)
    bl = jnp.logical_not(row_top) & col_left
    br = jnp.logical_not(row_top) & jnp.logical_not(col_left)
    al0, al1 = s.aligned[0], s.aligned[1]
    mid, top, low = swapped(s.staggered[0]), swapped(s.staggered[1]), swapped(s.carried[...])
    zero = jnp.zeros((L, L), f32)

    def pick(*items):
        value = zero
        for where, block in items:
            value = jnp.where(where, block, value)
        return value

    own = jnp.where(
        is_low, mid + pick((tl, al1), (br, al0)), pick((tl, al0 + low), (br, al1 + top)))
    beside = jnp.where(is_low, pick((tr, al0), (bl, al1)), pick((tr, al1), (bl, al0)))
    across = pick((tr, top), (bl, low))
    for k, value in enumerate((own, across, beside)):
        hi, lo = parted(value)
        s.gain[k * L : (k + 1) * L, :L] = hi
        s.gain[k * L : (k + 1) * L, L:] = lo

    inner_forward(0)
    inner_back(0)

    def rz_part(index, carry):
        at = span(index)
        return carry + eights(s.spec[0, at, :] * (s.mixed[0, at, :] * weight_of(at)))

    s.part[0, 0] = lax.fori_loop(0, W // 128, rz_part, jnp.zeros((8, L), f32))

    recv_all(s.row_in, s.rrow)
    wait_edges(0)
    north_col, south_col = column_of(0, 0), column_of(0, 1)
    for k in range(2):
        s.wet[k, 8 + length : 9 + length, :] = s.row_in[0, k, 0:1, :]
        s.east[k, 7:8, :] = s.row_in[2, k, last_row : last_row + 1, :] * s.wet[k, 8:9, :]
    lane = lax.broadcasted_iota(jnp.int32, (128, L), 1)
    first_lane, last_lane = lane == 0, lane == L - 1
    for b in range(blocks):
        at, at8, at9 = pl.ds(128 * b, 128), pl.ds(128 * b + 8, 128), pl.ds(128 * b + 9, 128)
        wet = [s.wet[k, at8, :] for k in range(2)]
        east = [s.east_wet[k, at, :] * s.wet[k, at9, :] for k in range(2)]
        moved = [pltpu.roll(value, L - 1, 1) for value in wet]
        beyond = jnp.broadcast_to(north_col[:, b : b + 1], (128, L))
        north = [
            s.north[0, at, :] * jnp.where(last_lane, moved[1], moved[0]),
            s.north[1, at, :] * jnp.where(last_lane, beyond, moved[1]),
        ]
        moved = [pltpu.roll(value, 1, 1) for value in north]
        beyond = jnp.broadcast_to(south_col[:, b : b + 1], (128, L))
        south = [
            jnp.where(first_lane, beyond * wet[0], moved[0]),
            jnp.where(first_lane, moved[0], moved[1]),
        ]
        for k in range(2):
            s.east[k, at8, :] = east[k]
            s.north[k, at, :] = north[k]
            s.south[k, at, :] = south[k]
    def make_diag(start, count):
        at, at8 = pl.ds(start, count), eight_on(start, count)
        for k in range(2):
            wet = s.wet[k, at8, :]
            own = (1.0 - wet) + wet * s.selfc[at, k * L : (k + 1) * L]
            s.diag[k, at, :] = own + s.diag[k, at, :]

    for b in range(blocks):
        at, at8, at7 = pl.ds(128 * b, 128), pl.ds(128 * b + 8, 128), pl.ds(128 * b + 7, 128)
        for k in range(2):
            s.diag[k, at, :] = (
                (s.east[k, at8, :] + s.east[k, at7, :]) + (s.north[k, at, :] + s.south[k, at, :]))
    s.diag[:, length:R, :] = jnp.zeros((2, R - length, L), f32)
    loop_rows(make_diag)
    for t in range(2):
        for g in range(2):
            if R > used:
                s.got4[t, g, used:, :] = jnp.zeros((R - used, L), f32)

    drain(2)
    outer_back(0, 0, True)
    outer_back(0, 1, True)
    wait_back(0, 0)
    wait_back(0, 1)
    wait_rows()

    def fields_of(t, at, count):
        a, b = s.got4[t, 0, at, :], s.got4[t, 1, at, :]
        mask = lanes_left(count)
        return jnp.where(mask, b, a), jnp.where(mask, a, b)

    def make_field(index):
        at8 = shifted(index)
        for k, value in enumerate(fields_of(0, span(index), 128)):
            s.field[k, at8, :] = s.wet[k, at8, :] * value

    loop(blocks, make_field)
    take_edges(1, s.field.at[0], s.field.at[1], (8, 8))
    send_edges(1)
    mask1 = lanes_left(1)
    for way, (row, source) in enumerate(((0, 0), (last_row, 1))):
        a, b = s.ew[way, 0, row : row + 1, :], s.ew[way, 1, row : row + 1, :]
        for k, value in enumerate((jnp.where(mask1, b, a), jnp.where(mask1, a, b))):
            at = 8 + length if way == 0 else 7
            s.field[k, at : at + 1, :] = s.row_in[source, k, row : row + 1, :] * value

    curvature = jnp.zeros((8, L), f32)
    for b in range(blocks):
        at, at8 = pl.ds(128 * b, 128), pl.ds(128 * b + 8, 128)
        at7, at9 = pl.ds(128 * b + 7, 128), pl.ds(128 * b + 9, 128)
        here = [s.field[k, at8, :] for k in range(2)]
        up = [pltpu.roll(value, L - 1, 1) for value in here]
        down = [pltpu.roll(value, 1, 1) for value in here]
        up = [jnp.where(last_lane, up[1], up[0]), jnp.where(last_lane, 0.0, up[1])]
        down = [jnp.where(first_lane, 0.0, down[0]), jnp.where(first_lane, down[0], down[1])]
        image = []
        for k in range(2):
            value = s.diag[k, at, :] * here[k]
            value = value - s.east[k, at8, :] * s.field[k, at9, :]
            value = value - s.east[k, at7, :] * s.field[k, at7, :]
            value = value - s.north[k, at, :] * up[k]
            value = value - s.south[k, at, :] * down[k]
            if 128 * (b + 1) > length:
                row = lax.broadcasted_iota(jnp.int32, (128, L), 0)
                value = jnp.where(row < length - 128 * b, value, 0.0)
            image.append(value)
            curvature = curvature + eights(here[k] * image[k])
        s.xs[1, 0, at, :], s.xs[1, 1, at, :] = groups_of(*image)

    send_phase1(1, 0)
    drain(2)
    wait_edges(1)
    north_col, south_col = column_of(1, 0), column_of(1, 1)
    for b in range(blocks):
        at, at8 = pl.ds(128 * b, 128), pl.ds(128 * b + 8, 128)
        south = s.south[0, at, :] * jnp.broadcast_to(south_col[:, b : b + 1], (128, L))
        north = s.north[1, at, :] * jnp.broadcast_to(north_col[:, b : b + 1], (128, L))
        extra = jnp.where(first_lane, south, jnp.where(last_lane, north, 0.0))
        s.xs[1, 1, at, :] = s.xs[1, 1, at, :] - extra
        here = jnp.where(first_lane, s.field[0, at8, :], s.field[1, at8, :])
        curvature = curvature - eights(here * extra)
    send_phase1(1, 1)
    s.part[0, 1] = curvature
    reduce_send(0)

    outer_forward(1, 0)
    outer_forward(1, 1)
    reduce_middle(0)
    inner_forward(1)
    rz_now, bend = reduce_end(0)
    alpha = rz_now / bend

    def rz_next_part(index, carry):
        at = span(index)
        spectrum = s.spec[0, at, :] - alpha * s.spec[1, at, :]
        mixed = s.mixed[0, at, :] - alpha * s.mixed[1, at, :]
        return carry + eights(spectrum * (mixed * weight_of(at)))

    def send_rz_next():
        s.part[1, 0] = lax.fori_loop(0, W // 128, rz_next_part, jnp.zeros((8, L), f32))
        s.part[1, 1] = jnp.zeros((8, L), f32)
        reduce_send(1)

    inner_back(1, send_rz_next)

    drain(3)
    outer_back(1, 0, False)
    outer_back(1, 1, False)
    reduce_middle(1)

    def first_outputs(start, count):
        at, at8 = pl.ds(start, count), eight_on(start, count)
        mask = lanes_left(count)
        rest = [s.xs[0, g, at, :] - alpha * s.xs[1, g, at, :] for g in range(2)]
        s.out[1, at, :L] = jnp.where(mask, rest[1], rest[0])
        s.out[1, at, L:] = jnp.where(mask, rest[0], rest[1])
        for k in range(2):
            s.out[0, at, k * L : (k + 1) * L] = alpha * s.field[k, at8, :]

    loop_rows(first_outputs)
    stores = [
        pltpu.make_async_copy(s.out.at[k], ref, s.store.at[k])
        for k, ref in enumerate((solution_ref, residual_ref, direction_ref))
    ]
    stores[0].start()
    stores[1].start()
    rz_next, _ = reduce_end(1)
    beta = rz_next / rz_now
    wait_back(1, 0)
    drain()
    wait_back(1, 1)

    def last_output(start, count):
        at, at8 = pl.ds(start, count), eight_on(start, count)
        for k, value in enumerate(fields_of(1, at, count)):
            first = s.field[k, at8, :]
            second = first - alpha * (s.wet[k, at8, :] * value)
            s.out[2, at, k * L : (k + 1) * L] = second + beta * first

    loop_rows(last_output)
    stores[2].start()
    for store in stores:
        store.wait()
    drain()


def finish_kernel(*refs):
    ins, outs, held, arrived, left = refs[:3], refs[3:6], refs[6], refs[7], refs[8]
    gets = [pltpu.make_async_copy(ref, held.at[k], arrived.at[k]) for k, ref in enumerate(ins)]
    puts = [pltpu.make_async_copy(held.at[k], ref, left.at[k]) for k, ref in enumerate(outs)]
    for get in gets:
        get.start()
    for get, put in zip(gets, puts):
        get.wait()
        put.start()
    for put in puts:
        put.wait()


def local(
    surface_forcing,
    ocean_mask,
    self_coupling,
    east_coupling,
    north_coupling,
    zonal_weight,
    aligned_inverse,
    staggered_inverse,
):
    groups, bands = lax.axis_size("lon"), lax.axis_size("lat")
    length, columns = surface_forcing.shape
    block = aligned_inverse.shape[1]
    assert columns == 2 * block and block == 128 and groups % 4 == 0
    chunk = -(-length // (8 * groups)) * 8
    padded = groups * chunk
    while 2 * padded % 128:
        chunk, padded = chunk + 8, padded + 8 * groups
    plan = Plan(groups, bands, length, columns, block, (chunk, padded))
    assert plan.rows <= 1024
    matrix, waves = inner_tables(groups, length, padded)
    lanes = np.repeat(waves[:, :, None], block, axis=2)
    scratch = plan.scratch()
    anywhere = pl.BlockSpec(memory_space=pl.ANY)
    shape = jax.ShapeDtypeStruct((length, columns), jnp.float32)
    outs = pl.pallas_call(
        functools.partial(kernel, plan, tuple(scratch)),
        out_shape=(shape,) * 3,
        in_specs=[anywhere] * 10,
        out_specs=(anywhere,) * 3,
        scratch_shapes=list(scratch.values()),
        compiler_params=pltpu.CompilerParams(
            collective_id=0, has_side_effects=True, vmem_limit_bytes=61 * 2**20
        ),
        name="step",
    )(
        surface_forcing, ocean_mask, self_coupling, east_coupling, north_coupling,
        zonal_weight[None, :], aligned_inverse, staggered_inverse,
        jnp.asarray(matrix), jnp.asarray(lanes),
    )
    return pl.pallas_call(
        finish_kernel,
        out_shape=(shape,) * 3,
        in_specs=[anywhere] * 3,
        out_specs=(anywhere,) * 3,
        scratch_shapes=[
            pltpu.VMEM((3, length, columns), jnp.float32),
            pltpu.SemaphoreType.DMA((3,)),
            pltpu.SemaphoreType.DMA((3,)),
        ],
        name="finish",
    )(*outs)


def solution(mesh):
    grid = P("lon", "lat")
    stack = P("lat", None, None)
    return jax.shard_map(
        local,
        mesh=mesh,
        in_specs=(grid, grid, grid, grid, grid, P("lat"), stack, stack),
        out_specs=(grid, grid, grid),
        check_vma=False,
    )
```
